512 devices in a mesh: cell: 64 (over x, z, core), grp: 8 (over y).
Axes of the slice: x: 4, y: 8, z: 8, core: 2. Of those that a mesh axis runs over, the one named last changes fastest.
Arguments:
- atom_sites: float32 [3, 262144], P(None, ('cell', 'grp')), may hold values from 0 to 64, as said below
- grid_points: float32 [3, 196608], P(None, ('cell', 'grp')), may hold values from 0 to 64, as said below
- dipole_guess: float32 [3, 262144], P(None, ('cell', 'grp')), may hold values from -2 to 2
- fixed_field: float32 [3, 262144], P(None, ('cell', 'grp')), may hold values from -1800 to 1800
- polarisability: float32 [262144], P(('cell', 'grp')), may hold values from 0.0005 to 0.002
- base_charge: float32 [196608], P(('cell', 'grp')), may hold values from -12 to 12
- response: float32 [196608], P(('cell', 'grp')), may hold values from 0.02 to 0.2
- near_blocks: int32 [2048, 8], P(('cell', 'grp')), may hold values from 0 to 95, as said below
- grid_blocks: int32 [2048, 4], P(('cell', 'grp')), may hold values from 0 to 71, as said below
- source_blocks: int32 [1536, 8], P(('cell', 'grp')), may hold values from 0 to 95, as said below
Outputs:
- dipoles: float32 [3, 262144], P(None, ('cell', 'grp'))
- qm_charges: float32 [196608], P(('cell', 'grp'))
The draws below stay inside these ranges and needn't reach their ends.
Inputs may be any that keep to these rules, and one draw needn't show every extreme that they name: `atom_sites`: atom a has first coordinate in [c, c + 1) with c = a // 4096, the other two in [0, 1). `grid_points`: grid point g has first coordinate in [c, c + 1) with c = g // 3072, the other two in [0, 1). `near_blocks`: each row holds 8 distinct MM window indices, never the block's own index 32 + b % 32. `grid_blocks`: each row holds 4 distinct grid window indices. `source_blocks`: each row holds 8 distinct MM window indices.
All inputs are finite; a program needn't handle non-finite values.
Results may differ from the reference program's by a relative error of at most 0.0003.
Values sent between devices are 32-bit elements; how exact they have to be, the bound alone decides.
No kernel may reach another device: no remote copies, remote signals or barrier semaphores. Data moves between devices by JAX's collectives and lax.ppermute only.
A program may use at most 64 MiB of HBM per device.

```python
import math
import jax
import jax.numpy as jnp
from jax import lax

BLOCK = 128
NB = 8
NQ = 4
NM = 8
ITERS = 3
CELLS = 64
CELL_BLK = 32
CELL_GBLK = 24
CELL_ATOMS = 4096
CELL_GRID = 3072
BLOCKS = 2048
GBLOCKS = 1536
ATOMS = 262144
GRID = 196608


def place_points(key, per_cell):
    uniform_unit = jax.random.uniform(key, (3, CELLS * per_cell), jnp.float32)
    shift_x = (jnp.arange(CELLS * per_cell, dtype=jnp.int32) // per_cell).astype(jnp.float32)
    return jnp.stack([uniform_unit[0] + shift_x, uniform_unit[1], uniform_unit[2]])


def window_lists(key, row_count, span, picks, cell_rows, exclude_own):
    scores = jax.random.randint(key, (row_count, span), 0, 1 << 20, dtype=jnp.int32) * span
    scores = scores + jnp.arange(span, dtype=jnp.int32)[None, :]
    if exclude_own:
        own_rows = cell_rows + jnp.arange(row_count, dtype=jnp.int32) % cell_rows
        scores = jnp.where(jnp.arange(span, dtype=jnp.int32)[None, :] == own_rows[:, None], -1, scores)
    return lax.top_k(scores, picks)[1].astype(jnp.int32)


def draw_atom_sites(key, part):
    return place_points(jax.random.fold_in(key, 11), CELL_ATOMS)


def draw_grid_points(key, part):
    return place_points(jax.random.fold_in(key, 12), CELL_GRID)


def draw_near_blocks(key, part):
    return window_lists(jax.random.fold_in(key, 21), BLOCKS, 3 * CELL_BLK, NB, CELL_BLK, True)


def draw_grid_blocks(key, part):
    return window_lists(jax.random.fold_in(key, 22), BLOCKS, 3 * CELL_GBLK, NQ, CELL_GBLK, False)


def draw_source_blocks(key, part):
    return window_lists(jax.random.fold_in(key, 23), GBLOCKS, 3 * CELL_BLK, NM, CELL_BLK, False)


def level_of(own_key, dims, shards, low, top_value):
    def one(dim, blocks):
        steps = jax.random.uniform(jax.random.fold_in(jax.random.fold_in(own_key, 6), dim), (blocks,), jnp.float32, low / len(shards), top_value / len(shards))
        return jnp.repeat(jnp.exp(steps), dims[dim] // blocks).reshape((-1,) + (1,) * (len(dims) - dim - 1))

    gain = one(*shards[0])
    for cut in shards[1:]:
        gain = gain * one(*cut)
    return gain


def scatter_about(own_key, extent, deviation, bound, shards=(), kind=jnp.bfloat16):
    gain = level_of(own_key, extent, shards, -0.22, 0.18) if shards else 1.0
    values = jax.random.normal(own_key, extent, jnp.float32) * deviation * gain
    return jnp.minimum(jnp.maximum(values, -bound), bound).astype(kind)


def setup_inputs(seed: int = 0) -> dict:
    arg_keys = jax.random.split(jax.random.key(seed), 11)
    atom_sites = draw_atom_sites(jax.random.fold_in(arg_keys[10], 71), 0)
    grid_points = draw_grid_points(jax.random.fold_in(arg_keys[10], 71), 0)
    dipole_guess = scatter_about(arg_keys[2], (3, ATOMS), 0.3, 2.0, ((1, 512),), jnp.float32)
    fixed_field = scatter_about(arg_keys[3], (3, ATOMS), 300.0, 1800.0, ((1, 512),), jnp.float32)
    polarisability = jnp.clip(jnp.exp(math.log(0.002) - 1.3862944 * jax.random.uniform(arg_keys[4], (ATOMS,), jnp.float32) ** level_of(arg_keys[4], (ATOMS,), ((0, 512),), -0.2, 0.2)), 0.0005, 0.002)
    base_charge = scatter_about(arg_keys[5], (GRID,), 2.0, 12.0, ((0, 512),), jnp.float32)
    response = jnp.clip(jnp.exp(math.log(0.2) - 2.3025851 * jax.random.uniform(arg_keys[6], (GRID,), jnp.float32) ** level_of(arg_keys[6], (GRID,), ((0, 512),), -0.2, 0.2)), 0.02, 0.2)
    near_blocks = draw_near_blocks(jax.random.fold_in(arg_keys[10], 71), 0)
    grid_blocks = draw_grid_blocks(jax.random.fold_in(arg_keys[10], 71), 0)
    source_blocks = draw_source_blocks(jax.random.fold_in(arg_keys[10], 71), 0)
    return dict(atom_sites=atom_sites, grid_points=grid_points, dipole_guess=dipole_guess, fixed_field=fixed_field, polarisability=polarisability, base_charge=base_charge, response=response, near_blocks=near_blocks, grid_blocks=grid_blocks, source_blocks=source_blocks)


soften_sq = 0.04

def pick_tile(tile_set, slot_index):
    return lax.dynamic_index_in_dim(tile_set, slot_index, 1, keepdims=False)

def pair_geometry(targets, sources):
    delta_x = targets[0][:, None] - sources[0][None, :]
    delta_y = targets[1][:, None] - sources[1][None, :]
    delta_z = targets[2][:, None] - sources[2][None, :]
    inverse = 1.0 / jnp.sqrt(delta_x * delta_x + delta_y * delta_y + delta_z * delta_z + soften_sq)
    inv_cube = inverse * inverse * inverse
    return (delta_x, delta_y, delta_z, inv_cube, inv_cube * inverse * inverse)

def dipole_field(targets, sources, moments, keep_mask):
    delta_x, delta_y, delta_z, inv_cube, inv_fifth = pair_geometry(targets, sources)
    projected = moments[0][None, :] * delta_x + moments[1][None, :] * delta_y + moments[2][None, :] * delta_z
    radial = 3.0 * projected * inv_fifth * keep_mask
    direct = inv_cube * keep_mask
    return jnp.stack([lax.optimization_barrier(jnp.sum(radial * delta_x - moments[0][None, :] * direct, axis=1)), lax.optimization_barrier(jnp.sum(radial * delta_y - moments[1][None, :] * direct, axis=1)), lax.optimization_barrier(jnp.sum(radial * delta_z - moments[2][None, :] * direct, axis=1))])

def charge_field(targets, sources, charges):
    delta_x, delta_y, delta_z, inv_cube, inv_fifth = pair_geometry(targets, sources)
    weight = charges[None, :] * inv_cube
    return jnp.stack([lax.optimization_barrier(jnp.sum(weight * delta_x, axis=1)), lax.optimization_barrier(jnp.sum(weight * delta_y, axis=1)), lax.optimization_barrier(jnp.sum(weight * delta_z, axis=1))])

def dipole_potential(targets, sources, moments):
    delta_x, delta_y, delta_z, inv_cube, inv_fifth = pair_geometry(targets, sources)
    projected = moments[0][None, :] * delta_x + moments[1][None, :] * delta_y + moments[2][None, :] * delta_z
    return lax.optimization_barrier(jnp.sum(projected * inv_cube, axis=1))

def far_geometry(targets, cell_here, cell_count):
    centres = jnp.arange(cell_count, dtype=jnp.int32).astype(jnp.float32) + 0.5
    delta_x = targets[0][None, :] - centres[:, None]
    delta_y = targets[1][None, :] - 0.5
    delta_z = targets[2][None, :] - 0.5
    far_mask = (jnp.abs(jnp.arange(cell_count, dtype=jnp.int32) - cell_here) >= 2).astype(jnp.float32)[:, None]
    inverse = 1.0 / jnp.sqrt(delta_x * delta_x + delta_y * delta_y + delta_z * delta_z + soften_sq)
    inv_cube = inverse * inverse * inverse * far_mask
    return (delta_x, delta_y, delta_z, inv_cube, inv_cube * inverse * inverse)

def far_field(targets, cell_here, moments, charges):
    delta_x, delta_y, delta_z, inv_cube, inv_fifth = far_geometry(targets, cell_here, charges.shape[0])
    projected = moments[:, 0:1] * delta_x + moments[:, 1:2] * delta_y + moments[:, 2:3] * delta_z
    radial = 3.0 * projected * inv_fifth
    coulomb = charges[:, None] * inv_cube
    return jnp.stack([lax.optimization_barrier(jnp.sum(radial * delta_x - moments[:, 0:1] * inv_cube + coulomb * delta_x, axis=0)), lax.optimization_barrier(jnp.sum(radial * delta_y - moments[:, 1:2] * inv_cube + coulomb * delta_y, axis=0)), lax.optimization_barrier(jnp.sum(radial * delta_z - moments[:, 2:3] * inv_cube + coulomb * delta_z, axis=0))])

def far_potential(targets, cell_here, moments):
    delta_x, delta_y, delta_z, inv_cube, inv_fifth = far_geometry(targets, cell_here, moments.shape[0])
    projected = moments[:, 0:1] * delta_x + moments[:, 1:2] * delta_y + moments[:, 2:3] * delta_z
    return lax.optimization_barrier(jnp.sum(projected * inv_cube, axis=0))

def atom_block(targets, own_slot, near_list, grid_list, site_tiles, dipole_tiles, point_tiles, charge_tiles, cell_here, moments, charge_sums):
    tile_width = targets.shape[1]
    self_mask = 1.0 - jnp.eye(tile_width, dtype=jnp.float32)
    accumulated = dipole_field(targets, pick_tile(site_tiles, own_slot), pick_tile(dipole_tiles, own_slot), self_mask)

    def near_step(member, carried):
        other_slot = near_list[member]
        return carried + dipole_field(targets, pick_tile(site_tiles, other_slot), pick_tile(dipole_tiles, other_slot), 1.0)
    accumulated = lax.fori_loop(0, near_list.shape[0], near_step, accumulated)

    def grid_step(member, carried):
        other_slot = grid_list[member]
        return carried + charge_field(targets, pick_tile(point_tiles, other_slot), lax.dynamic_index_in_dim(charge_tiles, other_slot, 0, keepdims=False))
    accumulated = lax.fori_loop(0, grid_list.shape[0], grid_step, accumulated)
    return accumulated + far_field(targets, cell_here, moments, charge_sums)

def grid_block(targets, source_list, site_tiles, dipole_tiles, cell_here, dipole_sums):

    def near_step(member, carried):
        other_slot = source_list[member]
        return carried + dipole_potential(targets, pick_tile(site_tiles, other_slot), pick_tile(dipole_tiles, other_slot))
    accumulated = lax.fori_loop(0, source_list.shape[0], near_step, jnp.zeros((targets.shape[1],), jnp.float32))
    return accumulated + far_potential(targets, cell_here, dipole_sums)

def cell_table(dipoles, charges, grid_points):
    dipole_sums = lax.optimization_barrier(jnp.sum(dipoles.reshape(3, CELLS, CELL_ATOMS), axis=2)).T
    charge_cells = charges.reshape(CELLS, CELL_GRID)
    centres = jnp.stack([jnp.arange(CELLS, dtype=jnp.int32).astype(jnp.float32) + 0.5, jnp.full((CELLS,), 0.5, jnp.float32), jnp.full((CELLS,), 0.5, jnp.float32)])
    offsets = grid_points.reshape(3, CELLS, CELL_GRID) - centres[:, :, None]
    charge_sums = lax.optimization_barrier(jnp.sum(charge_cells, axis=1))
    grid_moments = lax.optimization_barrier(jnp.sum(charge_cells[None, :, :] * offsets, axis=2)).T
    return (dipole_sums, charge_sums, grid_moments)

def reference(atom_sites, grid_points, dipole_guess, fixed_field, polarisability, base_charge, response, near_blocks, grid_blocks, source_blocks):
    target_tiles = atom_sites.reshape(3, BLOCKS, BLOCK)
    grid_targets = grid_points.reshape(3, GBLOCKS, BLOCK)
    site_tiles = jnp.pad(target_tiles, ((0, 0), (CELL_BLK, CELL_BLK), (0, 0)))
    point_tiles = jnp.pad(grid_targets, ((0, 0), (CELL_GBLK, CELL_GBLK), (0, 0)))
    dipoles = dipole_guess
    charges = base_charge
    for iteration in range(ITERS):
        dipole_sums, charge_sums, grid_moments = cell_table(dipoles, charges, grid_points)
        moments = dipole_sums + grid_moments
        dipole_tiles = jnp.pad(dipoles.reshape(3, BLOCKS, BLOCK), ((0, 0), (CELL_BLK, CELL_BLK), (0, 0)))
        charge_tiles = jnp.pad(charges.reshape(GBLOCKS, BLOCK), ((CELL_GBLK, CELL_GBLK), (0, 0)))

        def one_atom_block(block_index):
            cell_here = block_index // CELL_BLK
            window_start = cell_here * CELL_BLK
            grid_start = cell_here * CELL_GBLK
            return atom_block(pick_tile(target_tiles, block_index), block_index - window_start + CELL_BLK, near_blocks[block_index], grid_blocks[block_index], lax.dynamic_slice_in_dim(site_tiles, window_start, 3 * CELL_BLK, 1), lax.dynamic_slice_in_dim(dipole_tiles, window_start, 3 * CELL_BLK, 1), lax.dynamic_slice_in_dim(point_tiles, grid_start, 3 * CELL_GBLK, 1), lax.dynamic_slice_in_dim(charge_tiles, grid_start, 3 * CELL_GBLK, 0), cell_here, moments, charge_sums)

        def one_grid_block(block_index):
            cell_here = block_index // CELL_GBLK
            window_start = cell_here * CELL_BLK
            return grid_block(pick_tile(grid_targets, block_index), source_blocks[block_index], lax.dynamic_slice_in_dim(site_tiles, window_start, 3 * CELL_BLK, 1), lax.dynamic_slice_in_dim(dipole_tiles, window_start, 3 * CELL_BLK, 1), cell_here, dipole_sums)
        induced_field = lax.map(one_atom_block, jnp.arange(BLOCKS, dtype=jnp.int32))
        induced_field = jnp.transpose(induced_field, (1, 0, 2)).reshape(3, ATOMS)
        potential = lax.map(one_grid_block, jnp.arange(GBLOCKS, dtype=jnp.int32)).reshape(GRID)
        dipoles = polarisability[None, :] * (fixed_field + induced_field)
        charges = base_charge - response * potential
    return (dipoles, charges)
```

```python
import functools

import jax
import jax.numpy as jnp
from jax import lax
from jax.experimental import pallas as pl
from jax.experimental.pallas import tpu as pltpu
from jax.sharding import Mesh, PartitionSpec as P

LANES = 128
ITERS = 3
SOFT = 0.04
X, Z, CORES, GROUPS = 4, 8, 2, 8
CHIPS = X * Z
MEMBERS = CORES * GROUPS
AB, GB = 4, 3
DYN = 16
FIRST = 40
SITE, POINT = 16, 28
OWN = 48
FIXED, POL, BASE, RESP = 21, 33, 37, 40

VM = pl.BlockSpec(memory_space=pltpu.VMEM)
SM = pl.BlockSpec(memory_space=pltpu.SMEM)


def out(*shape):
    return jax.ShapeDtypeStruct(shape, jnp.float32)


def call(kernel, outs, args, specs=None, flops=1_000_000, scratch=(), limit=8 << 20, name=None):
    return pl.pallas_call(
        kernel,
        out_shape=outs,
        in_specs=specs or [VM] * len(args),
        out_specs=jax.tree.map(lambda _: VM, outs),
        scratch_shapes=list(scratch),
        cost_estimate=pl.CostEstimate(flops=flops, bytes_accessed=1000, transcendentals=0),
        compiler_params=pltpu.CompilerParams(vmem_limit_bytes=limit),
        name=name,
    )(*args)


def block(ref, a, b):
    return ref[a : a + 1, b * LANES : (b + 1) * LANES]


def flat_block(ref, b):
    return ref[0:1, b * LANES : (b + 1) * LANES]


def begin_kernel(sites, points, guess, fixed, pol, base, resp, own, copies, rows):
    rows[...] = jnp.zeros_like(rows)
    own[...] = jnp.zeros_like(own)
    for b in range(AB):
        for a in range(3):
            rows[a * AB + b : a * AB + b + 1, :] = block(guess, a, b)
            s = block(sites, a, b)
            rows[SITE + a * AB + b : SITE + a * AB + b + 1, :] = s
            own[a * AB + b : a * AB + b + 1, :] = s
            own[FIXED + a * AB + b : FIXED + a * AB + b + 1, :] = block(fixed, a, b)
        own[POL + b : POL + b + 1, :] = flat_block(pol, b)
    for b in range(GB):
        for a in range(3):
            s = block(points, a, b)
            rows[POINT + a * GB + b : POINT + a * GB + b + 1, :] = s
            own[12 + a * GB + b : 12 + a * GB + b + 1, :] = s
        rows[12 + b : 13 + b, :] = flat_block(base, b)
        own[BASE + b : BASE + b + 1, :] = flat_block(base, b)
        own[RESP + b : RESP + b + 1, :] = flat_block(resp, b)
    everything = rows[...]
    for i in range(MEMBERS):
        copies[i] = everything


def position():
    core = lax.axis_index("core")
    return core, (lax.axis_index("x") * Z + lax.axis_index("z")) * CORES


def sums_kernel(dyn, static, far, halo, table):
    core, first_cell = position()
    table[...] = jnp.zeros_like(table)
    for k in range(CORES):
        dipoles = [jnp.zeros((AB, LANES), jnp.float32) for _ in range(3)]
        charge = jnp.zeros((GB, LANES), jnp.float32)
        offset = [jnp.zeros((GB, LANES), jnp.float32) for _ in range(3)]
        centre = [(first_cell + k).astype(jnp.float32) + 0.5, 0.5, 0.5]
        for g in range(GROUPS):
            m = k * GROUPS + g
            q = dyn[m, 12 : 12 + GB, :]
            charge = charge + q
            for a in range(3):
                dipoles[a] = dipoles[a] + dyn[m, a * AB : (a + 1) * AB, :]
                p = static[m, POINT + a * GB : POINT + (a + 1) * GB, :]
                offset[a] = offset[a] + q * (p - centre[a])
        for a in range(3):
            p = jnp.sum(dipoles[a], axis=0, keepdims=True)
            table[k * 8 + a : k * 8 + a + 1, :] = p
            table[k * 8 + 4 + a : k * 8 + 5 + a, :] = p + jnp.sum(offset[a], axis=0, keepdims=True)
        table[k * 8 + 3 : k * 8 + 4, :] = jnp.sum(charge, axis=0, keepdims=True)
    totals = jnp.broadcast_to(jnp.sum(table[...], axis=1, keepdims=True), (16, LANES))
    diagonal = lax.broadcasted_iota(jnp.int32, (16, LANES), 0) == lax.broadcasted_iota(
        jnp.int32, (16, LANES), 1
    )
    row = jnp.sum(jnp.where(diagonal, totals, 0.0), axis=0, keepdims=True)
    for i in range(CHIPS):
        far[i] = row
    halo[...] = dyn[pl.ds(core * GROUPS, GROUPS)]


def geometry(t, s):
    dx, dy, dz = (t[a] - s[a] for a in range(3))
    inverse = lax.rsqrt(dx * dx + dy * dy + (dz * dz + SOFT))
    square = inverse * inverse
    return dx, dy, dz, inverse * square, square


CHUNK = 32


def near_kernel(
    near, grids, sources, own, dyn, dyn_halo, static, static_halo, result, columns, sums, moving, fixed
):
    core, _ = position()
    moving[0:MEMBERS] = dyn[:, 0:DYN, :]
    moving[MEMBERS:] = dyn_halo[:, 0:DYN, :]
    fixed[0:MEMBERS] = static[:, SITE:FIRST, :]
    fixed[MEMBERS:] = static_halo[:, SITE:FIRST, :]
    for r in range(3 * AB + 3 * GB):
        columns[r] = jnp.transpose(jnp.broadcast_to(own[r : r + 1, :], (LANES, LANES)))

    first, second, third = (
        jnp.where(core == 0, MEMBERS, 0),
        jnp.where(core == 0, 0, GROUPS),
        jnp.where(core == 0, GROUPS, MEMBERS),
    )

    def place(slot, blocks):
        per_cell = blocks * GROUPS
        cell = slot // per_cell
        inside = slot - cell * per_cell
        share = jnp.where(cell == 0, first, jnp.where(cell == 1, second, third))
        group = inside // blocks
        return share + group, inside - group * blocks

    def rows(ref, share, start, step):
        return [ref[share, pl.ds(start + a * step, 1), :] for a in range(3)]

    def dipole_terms(share, b):
        s = rows(fixed, share, b, AB)
        m = rows(moving, share, b, AB)
        return s, m, [3.0 * v for v in m]

    me = second + lax.axis_index("grp")

    def atom_chunk(step, carry):
        tb = step // (LANES // CHUNK)
        start = pl.multiple_of((step - tb * (LANES // CHUNK)) * CHUNK, CHUNK)
        t = [columns[a * AB + tb, pl.ds(start, CHUNK), :] for a in range(3)]
        acc = [jnp.zeros((CHUNK, LANES), jnp.float32) for _ in range(3)]
        for n in range(9):
            if n == 0:
                share, b = me, tb
            else:
                share, b = place(near[tb, n - 1], AB)
            s, m, m3 = dipole_terms(share, b)
            dx, dy, dz, cube, square = geometry(t, s)
            weight = (m3[0] * dx + m3[1] * dy + m3[2] * dz) * (cube * square)
            if n == 0:
                other = (
                    lax.broadcasted_iota(jnp.int32, (CHUNK, LANES), 0) + start
                ) != lax.broadcasted_iota(jnp.int32, (CHUNK, LANES), 1)
                cube = jnp.where(other, cube, 0.0)
                weight = jnp.where(other, weight, 0.0)
            acc = [acc[a] + (weight * d - m[a] * cube) for a, d in enumerate((dx, dy, dz))]
        for n in range(4):
            share, b = place(grids[tb, n], GB)
            s = rows(fixed, share, 12 + b, GB)
            q = moving[share, pl.ds(12 + b, 1), :]
            dx, dy, dz, cube, _ = geometry(t, s)
            weight = q * cube
            acc = [acc[a] + weight * d for a, d in enumerate((dx, dy, dz))]
        for a in range(3):
            sums[a * AB + tb, pl.ds(start, CHUNK), :] = acc[a]
        return carry

    def grid_chunk(step, carry):
        tb = step // (LANES // CHUNK)
        start = pl.multiple_of((step - tb * (LANES // CHUNK)) * CHUNK, CHUNK)
        t = [columns[12 + a * GB + tb, pl.ds(start, CHUNK), :] for a in range(3)]
        acc = jnp.zeros((CHUNK, LANES), jnp.float32)
        for n in range(8):
            share, b = place(sources[tb, n], AB)
            s = rows(fixed, share, b, AB)
            m = rows(moving, share, b, AB)
            dx, dy, dz, cube, _ = geometry(t, s)
            acc = acc + (m[0] * dx + m[1] * dy + m[2] * dz) * cube
        sums[12 + tb, pl.ds(start, CHUNK), :] = acc
        return carry

    lax.fori_loop(0, AB * (LANES // CHUNK), atom_chunk, 0)
    lax.fori_loop(0, GB * (LANES // CHUNK), grid_chunk, 0)
    for r in range(12 + GB):
        result[r : r + 1, :] = jnp.sum(jnp.transpose(sums[r]), axis=0, keepdims=True)
    result[15:16, :] = jnp.zeros((1, LANES), jnp.float32)


def far_terms(table, here, targets):
    totals = [[jnp.zeros((8, LANES), jnp.float32) for _ in range(4)] for _ in range(AB)]
    potential = [jnp.zeros((8, LANES), jnp.float32) for _ in range(GB)]
    for k in range(CORES):
        for v in range(CHIPS // 8):
            chip = lax.broadcasted_iota(jnp.int32, (8, LANES), 0) + v * 8
            cell = chip * CORES + k
            centre = cell.astype(jnp.float32) + 0.5
            mask = jnp.where(jnp.abs(cell - here) >= 2, 1.0, 0.0)
            part = table[v * 8 : (v + 1) * 8, :]
            p0, p1, p2, q, m0, m1, m2 = (
                jnp.broadcast_to(part[:, k * 8 + j : k * 8 + j + 1], (8, LANES)) for j in range(7)
            )
            for b in range(AB):
                x, dy, dz = targets[b]
                dx = x - centre
                inverse = lax.rsqrt(dx * dx + (dy * dy + (dz * dz + SOFT)))
                square = inverse * inverse
                cube = inverse * square * mask
                weight = 3.0 * (m0 * dx + m1 * dy + m2 * dz) * (cube * square) + q * cube
                acc = totals[b]
                totals[b] = [
                    acc[0] + (weight * dx - m0 * cube),
                    acc[1] + m1 * cube,
                    acc[2] + m2 * cube,
                    acc[3] + weight,
                ]
            for b in range(GB):
                x, dy, dz = targets[AB + b]
                dx = x - centre
                inverse = lax.rsqrt(dx * dx + (dy * dy + (dz * dz + SOFT)))
                cube = inverse * (inverse * inverse) * mask
                potential[b] = potential[b] + (p0 * dx + p1 * dy + p2 * dz) * cube
    fields = []
    for b in range(AB):
        _, dy, dz = targets[b]
        sx, sy, sz, sw = (jnp.sum(t, axis=0, keepdims=True) for t in totals[b])
        fields.append((sx, dy * sw - sy, dz * sw - sz))
    return fields, [jnp.sum(p, axis=0, keepdims=True) for p in potential]


def update_kernel(last, own, near, far, *refs):
    core, first_cell = position()
    targets = []
    for b in range(AB):
        targets.append((own[b : b + 1, :], own[AB + b : AB + b + 1, :] - 0.5, own[2 * AB + b : 2 * AB + b + 1, :] - 0.5))
    for b in range(GB):
        r = 12 + b
        targets.append((own[r : r + 1, :], own[r + GB : r + GB + 1, :] - 0.5, own[r + 2 * GB : r + 2 * GB + 1, :] - 0.5))
    fields, potential = far_terms(far[:, 0, :], first_cell + core, targets)
    if last:
        dipoles, charges = refs
    else:
        copies, rows = refs
        rows[15:16, :] = jnp.zeros((1, LANES), jnp.float32)
    for b in range(AB):
        pol = own[POL + b : POL + b + 1, :]
        for a in range(3):
            r = a * AB + b
            value = pol * (own[FIXED + r : FIXED + r + 1, :] + (near[r : r + 1, :] + fields[b][a]))
            if last:
                dipoles[a : a + 1, b * LANES : (b + 1) * LANES] = value
            else:
                rows[r : r + 1, :] = value
    for b in range(GB):
        value = own[BASE + b : BASE + b + 1, :] - own[RESP + b : RESP + b + 1, :] * (
            near[12 + b : 13 + b, :] + potential[b]
        )
        if last:
            charges[0:1, b * LANES : (b + 1) * LANES] = value
        else:
            rows[12 + b : 13 + b, :] = value
    if not last:
        everything = rows[...]
        for i in range(MEMBERS):
            copies[i] = everything


def swaps():
    pairs = []
    for c in range(1, CHIPS * CORES - 1, 2):
        for g in range(GROUPS):
            i, j = c * GROUPS + g, (c + 1) * GROUPS + g
            pairs += [(i, j), (j, i)]
    return pairs


def body(sites, points, guess, fixed, pol, base, resp, near, grids, sources):
    flat = lambda v: v.reshape(1, -1)
    own, copies = call(
        begin_kernel,
        (out(OWN, LANES), out(MEMBERS, FIRST, LANES)),
        (sites, points, guess, fixed, flat(pol), flat(base), flat(resp)),
        scratch=[pltpu.VMEM((FIRST, LANES), jnp.float32)],
        name="begin",
    )
    static = static_halo = None
    for iteration in range(ITERS):
        last = iteration == ITERS - 1
        height = FIRST if iteration == 0 else DYN
        dyn = lax.all_to_all(copies, ("core", "grp"), 0, 0, tiled=True)
        static = dyn if static is None else static
        far_out, halo_out = call(
            sums_kernel,
            (out(CHIPS, 1, LANES), out(GROUPS, height, LANES)),
            (dyn, static),
            scratch=[pltpu.VMEM((16, LANES), jnp.float32)],
            name="sums",
        )
        halo = lax.ppermute(halo_out, ("x", "z", "core", "grp"), swaps())
        far = lax.all_to_all(far_out, ("x", "z"), 0, 0, tiled=True)
        static_halo = halo if static_halo is None else static_halo
        near_field = call(
            near_kernel,
            out(16, LANES),
            (near, grids, sources, own, dyn, halo, static, static_halo),
            specs=[SM] * 3 + [VM] * 5,
            flops=40_000_000,
            scratch=[
                pltpu.VMEM((21, LANES, LANES), jnp.float32),
                pltpu.VMEM((15, LANES, LANES), jnp.float32),
                pltpu.VMEM((MEMBERS + GROUPS, DYN, LANES), jnp.float32),
                pltpu.VMEM((MEMBERS + GROUPS, FIRST - SITE, LANES), jnp.float32),
            ],
            limit=16 << 20,
            name="near",
        )
        if last:
            dipoles, charges = call(
                functools.partial(update_kernel, True),
                (out(3, AB * LANES), out(1, GB * LANES)),
                (own, near_field, far),
                name="finish",
            )
        else:
            copies = call(
                functools.partial(update_kernel, False),
                out(MEMBERS, DYN, LANES),
                (own, near_field, far),
                scratch=[pltpu.VMEM((DYN, LANES), jnp.float32)],
                name="update",
            )
    return dipoles, charges.reshape(-1)


def solution(mesh):
    fine = Mesh(mesh.devices.reshape(X, Z, CORES, GROUPS), ("x", "z", "core", "grp"))
    every = ("x", "z", "core", "grp")
    return jax.shard_map(
        body,
        mesh=fine,
        in_specs=(P(None, every),) * 4 + (P(every),) * 3 + (P(every, None),) * 3,
        out_specs=(P(None, every), P(every)),
        check_vma=False,
    )
```

```python
import functools

import jax
import jax.numpy as jnp
from jax import lax
from jax.experimental import pallas as pl
from jax.experimental.pallas import tpu as pltpu
from jax.sharding import Mesh, PartitionSpec as P


LANES = 128
ITERS = 3
SOFT = 0.04
X, Z, CORES, GROUPS = 4, 8, 2, 8
CHIPS = X * Z
MEMBERS = CORES * GROUPS
AB, GB = 4, 3
DYN = 16
FIRST = 40
SITE, POINT = 16, 28
OWN = 48
FIXED, POL, BASE, RESP = 21, 33, 37, 40

VM = pl.BlockSpec(memory_space=pltpu.VMEM)
SM = pl.BlockSpec(memory_space=pltpu.SMEM)
ANY = pl.BlockSpec(memory_space=pl.ANY)


def out(*shape):
    return jax.ShapeDtypeStruct(shape, jnp.float32)


def call(kernel, outs, args, specs=None, flops=1_000_000, scratch=(), limit=8 << 20):
    return pl.pallas_call(
        kernel,
        out_shape=outs,
        in_specs=specs or [VM] * len(args),
        out_specs=jax.tree.map(lambda _: VM, outs),
        scratch_shapes=list(scratch),
        cost_estimate=pl.CostEstimate(flops=flops, bytes_accessed=1000, transcendentals=0),
        compiler_params=pltpu.CompilerParams(vmem_limit_bytes=limit),
    )(*args)


def share_sums(rows, own, table):
    core, first_cell = position()
    centre = [(first_cell + core).astype(jnp.float32) + 0.5, 0.5, 0.5]
    q = rows[12 : 12 + GB, :]
    table[7:8, :] = jnp.zeros((1, LANES), jnp.float32)
    table[3:4, :] = jnp.sum(q, axis=0, keepdims=True)
    for a in range(3):
        p = jnp.sum(rows[a * AB : (a + 1) * AB, :], axis=0, keepdims=True)
        d = q * (own[12 + a * GB : 12 + (a + 1) * GB, :] - centre[a])
        table[a : a + 1, :] = p
        table[4 + a : 5 + a, :] = p + jnp.sum(d, axis=0, keepdims=True)
    totals = jnp.broadcast_to(jnp.sum(table[...], axis=1, keepdims=True), (8, LANES))
    lane = lax.broadcasted_iota(jnp.int32, (8, LANES), 1)
    chosen = (lax.broadcasted_iota(jnp.int32, (8, LANES), 0) == (lane & 7)) & (lane < 16)
    rows[15:16, :] = jnp.sum(jnp.where(chosen, totals, 0.0), axis=0, keepdims=True)


def begin_kernel(
    sites, points, guess, fixed, pol, base, resp, own, copies, rows, table, in_sites, in_points, in_guess, in_fixed, sems
):
    pieces = [(sites, in_sites), (points, in_points), (guess, in_guess), (fixed, in_fixed)]
    for b in range(AB):
        pieces.append((pol.at[pl.ds(b * LANES, LANES)], own.at[POL + b]))
    for b in range(GB):
        pieces.append((base.at[pl.ds(b * LANES, LANES)], own.at[BASE + b]))
        pieces.append((resp.at[pl.ds(b * LANES, LANES)], own.at[RESP + b]))
    moves = [pltpu.make_async_copy(src, dst, sems.at[i]) for i, (src, dst) in enumerate(pieces)]
    for move in moves:
        move.start()
    rows[37:40, :] = jnp.zeros((3, LANES), jnp.float32)
    own[43:48, :] = jnp.zeros((5, LANES), jnp.float32)
    for move in moves:
        move.wait()
    for b in range(AB):
        lanes = slice(b * LANES, (b + 1) * LANES)
        for a in range(3):
            r = a * AB + b
            s = in_sites[a : a + 1, lanes]
            rows[r : r + 1, :] = in_guess[a : a + 1, lanes]
            rows[SITE + r : SITE + r + 1, :] = s
            own[r : r + 1, :] = s
            own[FIXED + r : FIXED + r + 1, :] = in_fixed[a : a + 1, lanes]
    for b in range(GB):
        lanes = slice(b * LANES, (b + 1) * LANES)
        for a in range(3):
            r = a * GB + b
            s = in_points[a : a + 1, lanes]
            rows[POINT + r : POINT + r + 1, :] = s
            own[12 + r : 13 + r, :] = s
        rows[12 + b : 13 + b, :] = own[BASE + b : BASE + b + 1, :]
    share_sums(rows, own, table)
    everything = rows[...]
    for i in range(MEMBERS):
        copies[i] = everything


def position():
    core = lax.axis_index("core")
    return core, (lax.axis_index("x") * Z + lax.axis_index("z")) * CORES


def sums_kernel(dyn, far, halo):
    core, _ = position()
    totals = []
    for k in range(CORES):
        total = dyn[k * GROUPS, 15:16, :]
        for g in range(1, GROUPS):
            total = total + dyn[k * GROUPS + g, 15:16, :]
        totals.append(total)
    lane = lax.broadcasted_iota(jnp.int32, (1, LANES), 1)
    row = jnp.where(lane < 8, totals[0], totals[1])
    for i in range(CHIPS):
        far[i] = row
    halo[...] = dyn[pl.ds(core * GROUPS, GROUPS)]


def geometry(t, s):
    dx, dy, dz = (t[a] - s[a] for a in range(3))
    inverse = lax.rsqrt(dx * dx + dy * dy + (dz * dz + SOFT))
    square = inverse * inverse
    return dx, dy, dz, inverse * square, square


CHUNK = 128


def near_kernel(
    near, grids, sources, own, dyn, dyn_halo, static, static_halo, result, columns, sums, moving, fixed
):
    core, _ = position()
    moving[0:MEMBERS] = dyn[:, 0:DYN, :]
    moving[MEMBERS:] = dyn_halo[:, 0:DYN, :]
    fixed[0:MEMBERS] = static[:, SITE:FIRST, :]
    fixed[MEMBERS:] = static_halo[:, SITE:FIRST, :]
    for r in range(3 * AB + 3 * GB):
        columns[r] = jnp.transpose(jnp.broadcast_to(own[r : r + 1, :], (LANES, LANES)))

    first, second, third = (
        jnp.where(core == 0, MEMBERS, 0),
        jnp.where(core == 0, 0, GROUPS),
        jnp.where(core == 0, GROUPS, MEMBERS),
    )

    def place(slot, blocks):
        per_cell = blocks * GROUPS
        cell = slot // per_cell
        inside = slot - cell * per_cell
        share = jnp.where(cell == 0, first, jnp.where(cell == 1, second, third))
        group = inside // blocks
        return share + group, inside - group * blocks

    def rows(ref, share, start, step):
        return [ref[share, pl.ds(start + a * step, 1), :] for a in range(3)]

    def dipole_terms(share, b):
        s = rows(fixed, share, b, AB)
        m = rows(moving, share, b, AB)
        return s, m, [3.0 * v for v in m]

    me = second + lax.axis_index("grp")

    def atom_chunk(step, carry):
        tb = step // (LANES // CHUNK)
        start = pl.multiple_of((step - tb * (LANES // CHUNK)) * CHUNK, CHUNK)
        t = [columns[a * AB + tb, pl.ds(start, CHUNK), :] for a in range(3)]
        acc = [jnp.zeros((CHUNK, LANES), jnp.float32) for _ in range(3)]
        for n in range(9):
            if n == 0:
                share, b = me, tb
            else:
                share, b = place(near[tb, n - 1], AB)
            s, m, m3 = dipole_terms(share, b)
            dx, dy, dz, cube, square = geometry(t, s)
            weight = (m3[0] * dx + m3[1] * dy + m3[2] * dz) * (cube * square)
            if n == 0:
                other = (
                    lax.broadcasted_iota(jnp.int32, (CHUNK, LANES), 0) + start
                ) != lax.broadcasted_iota(jnp.int32, (CHUNK, LANES), 1)
                cube = jnp.where(other, cube, 0.0)
                weight = jnp.where(other, weight, 0.0)
            acc = [acc[a] + (weight * d - m[a] * cube) for a, d in enumerate((dx, dy, dz))]
        for n in range(4):
            share, b = place(grids[tb, n], GB)
            s = rows(fixed, share, 12 + b, GB)
            q = moving[share, pl.ds(12 + b, 1), :]
            dx, dy, dz, cube, _ = geometry(t, s)
            weight = q * cube
            acc = [acc[a] + weight * d for a, d in enumerate((dx, dy, dz))]
        for a in range(3):
            sums[a * AB + tb, pl.ds(start, CHUNK), :] = acc[a]
        return carry

    def grid_chunk(step, carry):
        tb = step // (LANES // CHUNK)
        start = pl.multiple_of((step - tb * (LANES // CHUNK)) * CHUNK, CHUNK)
        t = [columns[12 + a * GB + tb, pl.ds(start, CHUNK), :] for a in range(3)]
        acc = jnp.zeros((CHUNK, LANES), jnp.float32)
        for n in range(8):
            share, b = place(sources[tb, n], AB)
            s = rows(fixed, share, b, AB)
            m = rows(moving, share, b, AB)
            dx, dy, dz, cube, _ = geometry(t, s)
            acc = acc + (m[0] * dx + m[1] * dy + m[2] * dz) * cube
        sums[12 + tb, pl.ds(start, CHUNK), :] = acc
        return carry

    lax.fori_loop(0, AB * (LANES // CHUNK), atom_chunk, 0)
    lax.fori_loop(0, GB * (LANES // CHUNK), grid_chunk, 0)
    for r in range(12 + GB):
        result[r : r + 1, :] = jnp.sum(jnp.transpose(sums[r]), axis=0, keepdims=True)
    result[15:16, :] = jnp.zeros((1, LANES), jnp.float32)


VECTORS = CORES * CHIPS // 8


def far_terms(far, table, wide, here, own):
    for i in range(CHIPS):
        table[i : i + 1, :] = far[i]
    centres, masks = [], []
    for n in range(VECTORS):
        k, v = n // (CHIPS // 8), n % (CHIPS // 8)
        cell = (lax.broadcasted_iota(jnp.int32, (8, LANES), 0) + v * 8) * CORES + k
        centres.append(cell.astype(jnp.float32) + 0.5)
        masks.append(jnp.where(jnp.abs(cell - here) >= 2, 1.0, 0.0))
        part = table[v * 8 : (v + 1) * 8, :]
        for j in range(7):
            wide[n * 7 + j] = jnp.broadcast_to(part[:, k * 8 + j : k * 8 + j + 1], (8, LANES))

    def wide_row(r):
        return jnp.broadcast_to(own[r : r + 1, :], (8, LANES))

    fields, potential = [], []
    for b in range(AB + GB):
        atom = b < AB
        r, stride = (b, AB) if atom else (12 + b - AB, GB)
        x, dy, dz = wide_row(r), wide_row(r + stride) - 0.5, wide_row(r + 2 * stride) - 0.5
        across = dy * dy + (dz * dz + SOFT)
        sums = None
        for n in range(VECTORS):
            dx = x - centres[n]
            inverse = lax.rsqrt(dx * dx + across)
            square = inverse * inverse
            cube = inverse * square * masks[n]
            if atom:
                q, m0, m1, m2 = (wide[n * 7 + j] for j in (3, 4, 5, 6))
                weight = 3.0 * (m0 * dx + m1 * dy + m2 * dz) * (cube * square) + q * cube
                terms = [weight * dx - m0 * cube, m1 * cube, m2 * cube, weight]
            else:
                p0, p1, p2 = (wide[n * 7 + j] for j in (0, 1, 2))
                terms = [(p0 * dx + p1 * dy + p2 * dz) * cube]
            sums = terms if sums is None else [s + t for s, t in zip(sums, terms)]
        if atom:
            sx, sy, sz, sw = sums
            parts = [sx, dy * sw - sy, dz * sw - sz]
            fields.append([jnp.sum(t, axis=0, keepdims=True) for t in parts])
        else:
            potential.append(jnp.sum(sums[0], axis=0, keepdims=True))
    return fields, potential


def update_kernel(last, own, near, far, *refs):
    core, first_cell = position()
    if last:
        dipoles, charges, far_table, wide = refs
    else:
        copies, rows, table, far_table, wide = refs
    fields, potential = far_terms(far, far_table, wide, first_cell + core, own)
    for b in range(AB):
        pol = own[POL + b : POL + b + 1, :]
        for a in range(3):
            r = a * AB + b
            value = pol * (own[FIXED + r : FIXED + r + 1, :] + (near[r : r + 1, :] + fields[b][a]))
            if last:
                dipoles[a : a + 1, b * LANES : (b + 1) * LANES] = value
            else:
                rows[r : r + 1, :] = value
    for b in range(GB):
        value = own[BASE + b : BASE + b + 1, :] - own[RESP + b : RESP + b + 1, :] * (
            near[12 + b : 13 + b, :] + potential[b]
        )
        if last:
            charges[0:1, b * LANES : (b + 1) * LANES] = value
        else:
            rows[12 + b : 13 + b, :] = value
    if not last:
        share_sums(rows, own, table)
        everything = rows[...]
        for i in range(MEMBERS):
            copies[i] = everything


def swaps():
    pairs = []
    for c in range(1, CHIPS * CORES - 1, 2):
        for g in range(GROUPS):
            i, j = c * GROUPS + g, (c + 1) * GROUPS + g
            pairs += [(i, j), (j, i)]
    return pairs


def begin(sites, points, guess, fixed, pol, base, resp):
    return call(
        begin_kernel,
        (out(OWN, LANES), out(MEMBERS, FIRST, LANES)),
        (sites, points, guess, fixed, pol, base, resp),
        specs=[ANY] * 7,
        scratch=[
            pltpu.VMEM((FIRST, LANES), jnp.float32),
            pltpu.VMEM((8, LANES), jnp.float32),
            pltpu.VMEM((3, AB * LANES), jnp.float32),
            pltpu.VMEM((3, GB * LANES), jnp.float32),
            pltpu.VMEM((3, AB * LANES), jnp.float32),
            pltpu.VMEM((3, AB * LANES), jnp.float32),
            pltpu.SemaphoreType.DMA((4 + AB + 2 * GB,)),
        ],
        limit=60 << 20,
    )


def body(sites, points, guess, fixed, pol, base, resp, near, grids, sources):
    own, copies = begin(sites, points, guess, fixed, pol, base, resp)
    far_scratch = [
        pltpu.VMEM((CHIPS, LANES), jnp.float32),
        pltpu.VMEM((7 * VECTORS, 8, LANES), jnp.float32),
    ]
    static = static_halo = None
    for iteration in range(ITERS):
        last = iteration == ITERS - 1
        height = FIRST if iteration == 0 else DYN
        dyn = lax.all_to_all(copies, ("core", "grp"), 0, 0, tiled=True)
        static = dyn if static is None else static
        far_out, halo_out = call(
            sums_kernel, (out(CHIPS, 1, LANES), out(GROUPS, height, LANES)), (dyn,)
        )
        halo = lax.ppermute(halo_out, ("x", "z", "core", "grp"), swaps())
        far = lax.all_to_all(far_out, ("x", "z"), 0, 0, tiled=True)
        static_halo = halo if static_halo is None else static_halo
        near_field = call(
            near_kernel,
            out(16, LANES),
            (near, grids, sources, own, dyn, halo, static, static_halo),
            specs=[SM] * 3 + [VM] * 5,
            flops=40_000_000,
            scratch=[
                pltpu.VMEM((21, LANES, LANES), jnp.float32),
                pltpu.VMEM((15, LANES, LANES), jnp.float32),
                pltpu.VMEM((MEMBERS + GROUPS, DYN, LANES), jnp.float32),
                pltpu.VMEM((MEMBERS + GROUPS, FIRST - SITE, LANES), jnp.float32),
            ],
            limit=16 << 20,
        )
        if last:
            dipoles, charges = call(
                functools.partial(update_kernel, True),
                (out(3, AB * LANES), out(1, GB * LANES)),
                (own, near_field, far),
                scratch=far_scratch,
            )
        else:
            copies = call(
                functools.partial(update_kernel, False),
                out(MEMBERS, DYN, LANES),
                (own, near_field, far),
                scratch=[pltpu.VMEM((DYN, LANES), jnp.float32), pltpu.VMEM((8, LANES), jnp.float32)]
                + far_scratch,
            )
    return dipoles, charges.reshape(-1)


def solution(mesh):
    fine = Mesh(mesh.devices.reshape(X, Z, CORES, GROUPS), ("x", "z", "core", "grp"))
    every = ("x", "z", "core", "grp")
    return jax.shard_map(
        body,
        mesh=fine,
        in_specs=(P(None, every),) * 4 + (P(every),) * 3 + (P(every, None),) * 3,
        out_specs=(P(None, every), P(every)),
        check_vma=False,
    )
```

```python
import functools

import jax
import jax.numpy as jnp
from jax import lax
from jax.experimental import pallas as pl
from jax.experimental.pallas import tpu as pltpu
from jax.sharding import Mesh, PartitionSpec as P


LANES = 128
ITERS = 3
SOFT = 0.04
X, Z, CORES, GROUPS = 4, 8, 2, 8
CHIPS = X * Z
MEMBERS = CORES * GROUPS
AB, GB = 4, 3
DYN = 16
FIRST = 40
SITE, POINT = 16, 28
OWN = 48
FIXED, POL, BASE, RESP = 21, 33, 37, 40

VM = pl.BlockSpec(memory_space=pltpu.VMEM)
SM = pl.BlockSpec(memory_space=pltpu.SMEM)
ANY = pl.BlockSpec(memory_space=pl.ANY)


def out(*shape):
    return jax.ShapeDtypeStruct(shape, jnp.float32)


def call(kernel, outs, args, specs=None, flops=1_000_000, scratch=(), limit=8 << 20):
    return pl.pallas_call(
        kernel,
        out_shape=outs,
        in_specs=specs or [VM] * len(args),
        out_specs=jax.tree.map(lambda _: VM, outs),
        scratch_shapes=list(scratch),
        cost_estimate=pl.CostEstimate(flops=flops, bytes_accessed=1000, transcendentals=0),
        compiler_params=pltpu.CompilerParams(vmem_limit_bytes=limit),
    )(*args)


def share_sums(rows, own, table):
    core, first_cell = position()
    centre = [(first_cell + core).astype(jnp.float32) + 0.5, 0.5, 0.5]
    q = rows[12 : 12 + GB, :]
    table[7:8, :] = jnp.zeros((1, LANES), jnp.float32)
    table[3:4, :] = jnp.sum(q, axis=0, keepdims=True)
    for a in range(3):
        p = jnp.sum(rows[a * AB : (a + 1) * AB, :], axis=0, keepdims=True)
        d = q * (own[12 + a * GB : 12 + (a + 1) * GB, :] - centre[a])
        table[a : a + 1, :] = p
        table[4 + a : 5 + a, :] = p + jnp.sum(d, axis=0, keepdims=True)
    totals = jnp.broadcast_to(jnp.sum(table[...], axis=1, keepdims=True), (8, LANES))
    lane = lax.broadcasted_iota(jnp.int32, (8, LANES), 1)
    chosen = (lax.broadcasted_iota(jnp.int32, (8, LANES), 0) == (lane & 7)) & (lane < 16)
    rows[15:16, :] = jnp.sum(jnp.where(chosen, totals, 0.0), axis=0, keepdims=True)


def begin_kernel(
    sites, points, guess, fixed, pol, base, resp, own, copies, rows, table, in_sites, in_points, in_guess, in_fixed, sems
):
    pieces = [(sites, in_sites), (points, in_points), (guess, in_guess), (fixed, in_fixed)]
    for b in range(AB):
        pieces.append((pol.at[pl.ds(b * LANES, LANES)], own.at[POL + b]))
    for b in range(GB):
        pieces.append((base.at[pl.ds(b * LANES, LANES)], own.at[BASE + b]))
        pieces.append((resp.at[pl.ds(b * LANES, LANES)], own.at[RESP + b]))
    moves = [pltpu.make_async_copy(src, dst, sems.at[i]) for i, (src, dst) in enumerate(pieces)]
    for move in moves:
        move.start()
    rows[37:40, :] = jnp.zeros((3, LANES), jnp.float32)
    own[43:48, :] = jnp.zeros((5, LANES), jnp.float32)
    for move in moves:
        move.wait()
    for b in range(AB):
        lanes = slice(b * LANES, (b + 1) * LANES)
        for a in range(3):
            r = a * AB + b
            s = in_sites[a : a + 1, lanes]
            rows[r : r + 1, :] = in_guess[a : a + 1, lanes]
            rows[SITE + r : SITE + r + 1, :] = s
            own[r : r + 1, :] = s
            own[FIXED + r : FIXED + r + 1, :] = in_fixed[a : a + 1, lanes]
    for b in range(GB):
        lanes = slice(b * LANES, (b + 1) * LANES)
        for a in range(3):
            r = a * GB + b
            s = in_points[a : a + 1, lanes]
            rows[POINT + r : POINT + r + 1, :] = s
            own[12 + r : 13 + r, :] = s
        rows[12 + b : 13 + b, :] = own[BASE + b : BASE + b + 1, :]
    share_sums(rows, own, table)
    everything = rows[...]
    for i in range(MEMBERS):
        copies[i] = everything


def position():
    core = lax.axis_index("core")
    return core, (lax.axis_index("x") * Z + lax.axis_index("z")) * CORES


def sums_kernel(dyn, far, halo):
    core, _ = position()
    totals = []
    for k in range(CORES):
        total = dyn[k * GROUPS, 15:16, :]
        for g in range(1, GROUPS):
            total = total + dyn[k * GROUPS + g, 15:16, :]
        totals.append(total)
    lane = lax.broadcasted_iota(jnp.int32, (1, LANES), 1)
    row = jnp.where(lane < 8, totals[0], totals[1])
    for i in range(CHIPS):
        far[i] = row
    halo[...] = dyn[pl.ds(core * GROUPS, GROUPS)]


def geometry(t, s):
    dx, dy, dz = (t[a] - s[a] for a in range(3))
    inverse = lax.rsqrt(dx * dx + dy * dy + (dz * dz + SOFT))
    square = inverse * inverse
    return dx, dy, dz, inverse * square, square


CHUNK = 128


def near_kernel(
    near, grids, sources, own, dyn, dyn_halo, static, static_halo, result, columns, sums, moving, fixed
):
    core, _ = position()
    moving[0:MEMBERS] = dyn[:, 0:DYN, :]
    moving[MEMBERS:] = dyn_halo[:, 0:DYN, :]
    fixed[0:MEMBERS] = static[:, SITE:FIRST, :]
    fixed[MEMBERS:] = static_halo[:, SITE:FIRST, :]
    for r in range(3 * AB + 3 * GB):
        columns[r] = jnp.transpose(jnp.broadcast_to(own[r : r + 1, :], (LANES, LANES)))

    first, second, third = (
        jnp.where(core == 0, MEMBERS, 0),
        jnp.where(core == 0, 0, GROUPS),
        jnp.where(core == 0, GROUPS, MEMBERS),
    )

    def place(slot, blocks):
        per_cell = blocks * GROUPS
        cell = slot // per_cell
        inside = slot - cell * per_cell
        share = jnp.where(cell == 0, first, jnp.where(cell == 1, second, third))
        group = inside // blocks
        return share + group, inside - group * blocks

    def rows(ref, share, start, step):
        return [ref[share, pl.ds(start + a * step, 1), :] for a in range(3)]

    def dipole_terms(share, b):
        s = rows(fixed, share, b, AB)
        m = rows(moving, share, b, AB)
        return s, m, [3.0 * v for v in m]

    me = second + lax.axis_index("grp")

    def finished(r):
        result[r : r + 1, :] = jnp.sum(jnp.transpose(sums[r]), axis=0, keepdims=True)

    def atom_chunk(step, carry):
        tb = step // (LANES // CHUNK)
        start = 0
        t = [columns[a * AB + tb, pl.ds(start, CHUNK), :] for a in range(3)]
        acc = [jnp.zeros((CHUNK, LANES), jnp.float32) for _ in range(3)]
        for n in range(9):
            if n == 0:
                share, b = me, tb
            else:
                share, b = place(near[tb, n - 1], AB)
            s, m, m3 = dipole_terms(share, b)
            dx, dy, dz, cube, square = geometry(t, s)
            weight = (m3[0] * dx + m3[1] * dy + m3[2] * dz) * (cube * square)
            if n == 0:
                other = (
                    lax.broadcasted_iota(jnp.int32, (CHUNK, LANES), 0) + start
                ) != lax.broadcasted_iota(jnp.int32, (CHUNK, LANES), 1)
                cube = jnp.where(other, cube, 0.0)
                weight = jnp.where(other, weight, 0.0)
            acc = [acc[a] + (weight * d - m[a] * cube) for a, d in enumerate((dx, dy, dz))]
        for n in range(4):
            share, b = place(grids[tb, n], GB)
            s = rows(fixed, share, 12 + b, GB)
            q = moving[share, pl.ds(12 + b, 1), :]
            dx, dy, dz, cube, _ = geometry(t, s)
            weight = q * cube
            acc = [acc[a] + weight * d for a, d in enumerate((dx, dy, dz))]
        for a in range(3):
            sums[a * AB + tb, pl.ds(start, CHUNK), :] = acc[a]
        return carry

    def grid_chunk(step, carry):
        tb = step // (LANES // CHUNK)
        start = 0
        t = [columns[12 + a * GB + tb, pl.ds(start, CHUNK), :] for a in range(3)]
        acc = jnp.zeros((CHUNK, LANES), jnp.float32)
        for n in range(8):
            share, b = place(sources[tb, n], AB)
            s = rows(fixed, share, b, AB)
            m = rows(moving, share, b, AB)
            dx, dy, dz, cube, _ = geometry(t, s)
            acc = acc + (m[0] * dx + m[1] * dy + m[2] * dz) * cube
        sums[12 + tb, pl.ds(start, CHUNK), :] = acc
        return carry

    for step in range(AB):
        atom_chunk(step, 0)
        for a in range(3):
            finished(a * AB + step)
    for step in range(GB):
        grid_chunk(step, 0)
        finished(12 + step)
    result[15:16, :] = jnp.zeros((1, LANES), jnp.float32)


VECTORS = CORES * CHIPS // 8


def far_terms(far, table, wide, here, own):
    for i in range(CHIPS):
        table[i : i + 1, :] = far[i]
    centres, masks = [], []
    for n in range(VECTORS):
        k, v = n // (CHIPS // 8), n % (CHIPS // 8)
        cell = (lax.broadcasted_iota(jnp.int32, (8, LANES), 0) + v * 8) * CORES + k
        centres.append(cell.astype(jnp.float32) + 0.5)
        masks.append(jnp.where(jnp.abs(cell - here) >= 2, 1.0, 0.0))
        part = table[v * 8 : (v + 1) * 8, :]
        for j in range(7):
            wide[n * 7 + j] = jnp.broadcast_to(part[:, k * 8 + j : k * 8 + j + 1], (8, LANES))

    def wide_row(r):
        return jnp.broadcast_to(own[r : r + 1, :], (8, LANES))

    fields, potential = [], []
    for b in range(AB + GB):
        atom = b < AB
        r, stride = (b, AB) if atom else (12 + b - AB, GB)
        x, dy, dz = wide_row(r), wide_row(r + stride) - 0.5, wide_row(r + 2 * stride) - 0.5
        across = dy * dy + (dz * dz + SOFT)
        sums = None
        for n in range(VECTORS):
            dx = x - centres[n]
            inverse = lax.rsqrt(dx * dx + across)
            square = inverse * inverse
            cube = inverse * square * masks[n]
            if atom:
                q, m0, m1, m2 = (wide[n * 7 + j] for j in (3, 4, 5, 6))
                weight = 3.0 * (m0 * dx + m1 * dy + m2 * dz) * (cube * square) + q * cube
                terms = [weight * dx - m0 * cube, m1 * cube, m2 * cube, weight]
            else:
                p0, p1, p2 = (wide[n * 7 + j] for j in (0, 1, 2))
                terms = [(p0 * dx + p1 * dy + p2 * dz) * cube]
            sums = terms if sums is None else [s + t for s, t in zip(sums, terms)]
        if atom:
            sx, sy, sz, sw = sums
            parts = [sx, dy * sw - sy, dz * sw - sz]
            fields.append([jnp.sum(t, axis=0, keepdims=True) for t in parts])
        else:
            potential.append(jnp.sum(sums[0], axis=0, keepdims=True))
    return fields, potential


def update_kernel(last, own, near, far, *refs):
    core, first_cell = position()
    if last:
        dipoles, charges, far_table, wide = refs
    else:
        copies, rows, table, far_table, wide = refs
    fields, potential = far_terms(far, far_table, wide, first_cell + core, own)
    for b in range(AB):
        pol = own[POL + b : POL + b + 1, :]
        for a in range(3):
            r = a * AB + b
            value = pol * (own[FIXED + r : FIXED + r + 1, :] + (near[r : r + 1, :] + fields[b][a]))
            if last:
                dipoles[a : a + 1, b * LANES : (b + 1) * LANES] = value
            else:
                rows[r : r + 1, :] = value
    for b in range(GB):
        value = own[BASE + b : BASE + b + 1, :] - own[RESP + b : RESP + b + 1, :] * (
            near[12 + b : 13 + b, :] + potential[b]
        )
        if last:
            charges[b * LANES : (b + 1) * LANES] = value[0]
        else:
            rows[12 + b : 13 + b, :] = value
    if not last:
        share_sums(rows, own, table)
        everything = rows[...]
        for i in range(MEMBERS):
            copies[i] = everything


def swaps():
    pairs = []
    for c in range(1, CHIPS * CORES - 1, 2):
        for g in range(GROUPS):
            i, j = c * GROUPS + g, (c + 1) * GROUPS + g
            pairs += [(i, j), (j, i)]
    return pairs


def begin(sites, points, guess, fixed, pol, base, resp):
    return call(
        begin_kernel,
        (out(OWN, LANES), out(MEMBERS, FIRST, LANES)),
        (sites, points, guess, fixed, pol, base, resp),
        specs=[ANY] * 7,
        scratch=[
            pltpu.VMEM((FIRST, LANES), jnp.float32),
            pltpu.VMEM((8, LANES), jnp.float32),
            pltpu.VMEM((3, AB * LANES), jnp.float32),
            pltpu.VMEM((3, GB * LANES), jnp.float32),
            pltpu.VMEM((3, AB * LANES), jnp.float32),
            pltpu.VMEM((3, AB * LANES), jnp.float32),
            pltpu.SemaphoreType.DMA((4 + AB + 2 * GB,)),
        ],
        limit=60 << 20,
    )


def body(sites, points, guess, fixed, pol, base, resp, near, grids, sources):
    own, copies = begin(sites, points, guess, fixed, pol, base, resp)
    far_scratch = [
        pltpu.VMEM((CHIPS, LANES), jnp.float32),
        pltpu.VMEM((7 * VECTORS, 8, LANES), jnp.float32),
    ]
    static = static_halo = None
    for iteration in range(ITERS):
        last = iteration == ITERS - 1
        height = FIRST if iteration == 0 else DYN
        dyn = lax.all_to_all(copies, ("core", "grp"), 0, 0, tiled=True)
        static = dyn if static is None else static
        far_out, halo_out = call(
            sums_kernel, (out(CHIPS, 1, LANES), out(GROUPS, height, LANES)), (dyn,)
        )
        halo = lax.ppermute(halo_out, ("x", "z", "core", "grp"), swaps())
        far = lax.all_to_all(far_out, ("x", "z"), 0, 0, tiled=True)
        static_halo = halo if static_halo is None else static_halo
        near_field = call(
            near_kernel,
            out(16, LANES),
            (near, grids, sources, own, dyn, halo, static, static_halo),
            specs=[SM] * 3 + [VM] * 5,
            flops=40_000_000,
            scratch=[
                pltpu.VMEM((21, LANES, LANES), jnp.float32),
                pltpu.VMEM((15, LANES, LANES), jnp.float32),
                pltpu.VMEM((MEMBERS + GROUPS, DYN, LANES), jnp.float32),
                pltpu.VMEM((MEMBERS + GROUPS, FIRST - SITE, LANES), jnp.float32),
            ],
            limit=16 << 20,
        )
        if last:
            dipoles, charges = call(
                functools.partial(update_kernel, True),
                (out(3, AB * LANES), out(GB * LANES)),
                (own, near_field, far),
                scratch=far_scratch,
            )
        else:
            copies = call(
                functools.partial(update_kernel, False),
                out(MEMBERS, DYN, LANES),
                (own, near_field, far),
                scratch=[pltpu.VMEM((DYN, LANES), jnp.float32), pltpu.VMEM((8, LANES), jnp.float32)]
                + far_scratch,
            )
    return dipoles, charges


def solution(mesh):
    fine = Mesh(mesh.devices.reshape(X, Z, CORES, GROUPS), ("x", "z", "core", "grp"))
    every = ("x", "z", "core", "grp")
    return jax.shard_map(
        body,
        mesh=fine,
        in_specs=(P(None, every),) * 4 + (P(every),) * 3 + (P(every, None),) * 3,
        out_specs=(P(None, every), P(every)),
        check_vma=False,
    )
```

```python
import functools

import jax
import jax.numpy as jnp
from jax import lax
from jax.experimental import pallas as pl
from jax.experimental.pallas import tpu as pltpu
from jax.sharding import Mesh, PartitionSpec as P


LANES = 128
ITERS = 3
SOFT = 0.04
X, Z, CORES, GROUPS = 4, 8, 2, 8
CHIPS = X * Z
MEMBERS = CORES * GROUPS
AB, GB = 4, 3
DYN = 16
FIRST = 40
SITE, POINT = 16, 28
OWN = 48
FIXED, POL, BASE, RESP = 21, 33, 37, 40

VM = pl.BlockSpec(memory_space=pltpu.VMEM)
SM = pl.BlockSpec(memory_space=pltpu.SMEM)
ANY = pl.BlockSpec(memory_space=pl.ANY)


def out(*shape):
    return jax.ShapeDtypeStruct(shape, jnp.float32)


def call(kernel, outs, args, specs=None, flops=1_000_000, scratch=(), limit=8 << 20):
    return pl.pallas_call(
        kernel,
        out_shape=outs,
        in_specs=specs or [VM] * len(args),
        out_specs=jax.tree.map(lambda _: VM, outs),
        scratch_shapes=list(scratch),
        cost_estimate=pl.CostEstimate(flops=flops, bytes_accessed=1000, transcendentals=0),
        compiler_params=pltpu.CompilerParams(vmem_limit_bytes=limit),
    )(*args)


def share_sums(rows, own, table):
    core, first_cell = position()
    centre = [(first_cell + core).astype(jnp.float32) + 0.5, 0.5, 0.5]
    q = rows[12 : 12 + GB, :]
    table[7:8, :] = jnp.zeros((1, LANES), jnp.float32)
    table[3:4, :] = jnp.sum(q, axis=0, keepdims=True)
    for a in range(3):
        p = jnp.sum(rows[a * AB : (a + 1) * AB, :], axis=0, keepdims=True)
        d = q * (own[12 + a * GB : 12 + (a + 1) * GB, :] - centre[a])
        table[a : a + 1, :] = p
        table[4 + a : 5 + a, :] = p + jnp.sum(d, axis=0, keepdims=True)
    totals = jnp.broadcast_to(jnp.sum(table[...], axis=1, keepdims=True), (8, LANES))
    lane = lax.broadcasted_iota(jnp.int32, (8, LANES), 1)
    chosen = (lax.broadcasted_iota(jnp.int32, (8, LANES), 0) == (lane & 7)) & (lane < 16)
    rows[15:16, :] = jnp.sum(jnp.where(chosen, totals, 0.0), axis=0, keepdims=True)


def begin_kernel(
    sites, points, guess, fixed, pol, base, resp, own, copies, rows, table, in_sites, in_points, in_guess, in_fixed, sems
):
    pieces = [(sites, in_sites), (points, in_points), (guess, in_guess), (fixed, in_fixed)]
    for b in range(AB):
        pieces.append((pol.at[pl.ds(b * LANES, LANES)], own.at[POL + b]))
    for b in range(GB):
        pieces.append((base.at[pl.ds(b * LANES, LANES)], own.at[BASE + b]))
        pieces.append((resp.at[pl.ds(b * LANES, LANES)], own.at[RESP + b]))
    moves = [pltpu.make_async_copy(src, dst, sems.at[i]) for i, (src, dst) in enumerate(pieces)]
    for move in moves:
        move.start()
    rows[37:40, :] = jnp.zeros((3, LANES), jnp.float32)
    own[43:48, :] = jnp.zeros((5, LANES), jnp.float32)
    for move in moves:
        move.wait()
    for b in range(AB):
        lanes = slice(b * LANES, (b + 1) * LANES)
        for a in range(3):
            r = a * AB + b
            s = in_sites[a : a + 1, lanes]
            rows[r : r + 1, :] = in_guess[a : a + 1, lanes]
            rows[SITE + r : SITE + r + 1, :] = s
            own[r : r + 1, :] = s
            own[FIXED + r : FIXED + r + 1, :] = in_fixed[a : a + 1, lanes]
    for b in range(GB):
        lanes = slice(b * LANES, (b + 1) * LANES)
        for a in range(3):
            r = a * GB + b
            s = in_points[a : a + 1, lanes]
            rows[POINT + r : POINT + r + 1, :] = s
            own[12 + r : 13 + r, :] = s
        rows[12 + b : 13 + b, :] = own[BASE + b : BASE + b + 1, :]
    share_sums(rows, own, table)
    everything = rows[...]
    for i in range(MEMBERS):
        copies[i] = everything


def position():
    core = lax.axis_index("core")
    return core, (lax.axis_index("x") * Z + lax.axis_index("z")) * CORES


def sums_kernel(dyn, far, halo):
    core, _ = position()
    totals = []
    for k in range(CORES):
        total = None
        for g in range(GROUPS):
            part = dyn[MEMBERS - 1 - k * GROUPS - g, 15:16, :]
            total = part if total is None else total + part
        totals.append(total)
    lane = lax.broadcasted_iota(jnp.int32, (1, LANES), 1)
    row = jnp.where(lane < 8, totals[0], totals[1])
    for i in range(CHIPS):
        far[i] = row
    halo[...] = dyn[pl.ds((CORES - 1 - core) * GROUPS, GROUPS)]


def geometry(t, s):
    dx, dy, dz = (t[a] - s[a] for a in range(3))
    inverse = lax.rsqrt(dx * dx + dy * dy + (dz * dz + SOFT))
    square = inverse * inverse
    return dx, dy, dz, inverse * square, square


CHUNK = 128


def near_kernel(
    near, grids, sources, own, dyn, dyn_halo, static, static_halo, result, columns, sums, moving, fixed
):
    core, _ = position()
    for m in range(MEMBERS):
        moving[m] = dyn[MEMBERS - 1 - m, 0:DYN, :]
        fixed[m] = static[MEMBERS - 1 - m, SITE:FIRST, :]
    for g in range(GROUPS):
        moving[MEMBERS + g] = dyn_halo[GROUPS - 1 - g, 0:DYN, :]
        fixed[MEMBERS + g] = static_halo[GROUPS - 1 - g, SITE:FIRST, :]
    for r in range(3 * AB + 3 * GB):
        columns[r] = jnp.transpose(jnp.broadcast_to(own[r : r + 1, :], (LANES, LANES)))

    first, second, third = (
        jnp.where(core == 0, MEMBERS, 0),
        jnp.where(core == 0, 0, GROUPS),
        jnp.where(core == 0, GROUPS, MEMBERS),
    )

    def place(slot, blocks):
        per_cell = blocks * GROUPS
        cell = slot // per_cell
        inside = slot - cell * per_cell
        share = jnp.where(cell == 0, first, jnp.where(cell == 1, second, third))
        group = inside // blocks
        return share + group, inside - group * blocks

    def rows(ref, share, start, step):
        return [ref[share, pl.ds(start + a * step, 1), :] for a in range(3)]

    def dipole_terms(share, b):
        s = rows(fixed, share, b, AB)
        m = rows(moving, share, b, AB)
        return s, m, [3.0 * v for v in m]

    me = second + lax.axis_index("grp")

    def finished(r):
        result[r : r + 1, :] = jnp.sum(jnp.transpose(sums[r]), axis=0, keepdims=True)

    def atom_chunk(step, carry):
        tb = step // (LANES // CHUNK)
        start = 0
        t = [columns[a * AB + tb, pl.ds(start, CHUNK), :] for a in range(3)]
        acc = [jnp.zeros((CHUNK, LANES), jnp.float32) for _ in range(3)]
        for n in range(9):
            if n == 0:
                share, b = me, tb
            else:
                share, b = place(near[tb, n - 1], AB)
            s, m, m3 = dipole_terms(share, b)
            dx, dy, dz, cube, square = geometry(t, s)
            weight = (m3[0] * dx + m3[1] * dy + m3[2] * dz) * (cube * square)
            if n == 0:
                other = (
                    lax.broadcasted_iota(jnp.int32, (CHUNK, LANES), 0) + start
                ) != lax.broadcasted_iota(jnp.int32, (CHUNK, LANES), 1)
                cube = jnp.where(other, cube, 0.0)
                weight = jnp.where(other, weight, 0.0)
            acc = [acc[a] + (weight * d - m[a] * cube) for a, d in enumerate((dx, dy, dz))]
        for n in range(4):
            share, b = place(grids[tb, n], GB)
            s = rows(fixed, share, 12 + b, GB)
            q = moving[share, pl.ds(12 + b, 1), :]
            dx, dy, dz, cube, _ = geometry(t, s)
            weight = q * cube
            acc = [acc[a] + weight * d for a, d in enumerate((dx, dy, dz))]
        for a in range(3):
            sums[a * AB + tb, pl.ds(start, CHUNK), :] = acc[a]
        return carry

    def grid_chunk(step, carry):
        tb = step // (LANES // CHUNK)
        start = 0
        t = [columns[12 + a * GB + tb, pl.ds(start, CHUNK), :] for a in range(3)]
        acc = jnp.zeros((CHUNK, LANES), jnp.float32)
        for n in range(8):
            share, b = place(sources[tb, n], AB)
            s = rows(fixed, share, b, AB)
            m = rows(moving, share, b, AB)
            dx, dy, dz, cube, _ = geometry(t, s)
            acc = acc + (m[0] * dx + m[1] * dy + m[2] * dz) * cube
        sums[12 + tb, pl.ds(start, CHUNK), :] = acc
        return carry

    for step in range(AB):
        atom_chunk(step, 0)
        for a in range(3):
            finished(a * AB + step)
    for step in range(GB):
        grid_chunk(step, 0)
        finished(12 + step)
    result[15:16, :] = jnp.zeros((1, LANES), jnp.float32)


VECTORS = CORES * CHIPS // 8


def far_terms(far, table, wide, here, own):
    for i in range(CHIPS):
        table[i : i + 1, :] = far[CHIPS - 1 - i]
    centres, masks = [], []
    for n in range(VECTORS):
        k, v = n // (CHIPS // 8), n % (CHIPS // 8)
        cell = (lax.broadcasted_iota(jnp.int32, (8, LANES), 0) + v * 8) * CORES + k
        centres.append(cell.astype(jnp.float32) + 0.5)
        masks.append(jnp.where(jnp.abs(cell - here) >= 2, 1.0, 0.0))
        part = table[v * 8 : (v + 1) * 8, :]
        for j in range(7):
            wide[n * 7 + j] = jnp.broadcast_to(part[:, k * 8 + j : k * 8 + j + 1], (8, LANES))

    def wide_row(r):
        return jnp.broadcast_to(own[r : r + 1, :], (8, LANES))

    fields, potential = [], []
    for b in range(AB + GB):
        atom = b < AB
        r, stride = (b, AB) if atom else (12 + b - AB, GB)
        x, dy, dz = wide_row(r), wide_row(r + stride) - 0.5, wide_row(r + 2 * stride) - 0.5
        across = dy * dy + (dz * dz + SOFT)
        sums = None
        for n in range(VECTORS):
            dx = x - centres[n]
            inverse = lax.rsqrt(dx * dx + across)
            square = inverse * inverse
            cube = inverse * square * masks[n]
            if atom:
                q, m0, m1, m2 = (wide[n * 7 + j] for j in (3, 4, 5, 6))
                weight = 3.0 * (m0 * dx + m1 * dy + m2 * dz) * (cube * square) + q * cube
                terms = [weight * dx - m0 * cube, m1 * cube, m2 * cube, weight]
            else:
                p0, p1, p2 = (wide[n * 7 + j] for j in (0, 1, 2))
                terms = [(p0 * dx + p1 * dy + p2 * dz) * cube]
            sums = terms if sums is None else [s + t for s, t in zip(sums, terms)]
        if atom:
            sx, sy, sz, sw = sums
            parts = [sx, dy * sw - sy, dz * sw - sz]
            fields.append([jnp.sum(t, axis=0, keepdims=True) for t in parts])
        else:
            potential.append(jnp.sum(sums[0], axis=0, keepdims=True))
    return fields, potential


def update_kernel(last, own, near, far, *refs):
    core, first_cell = position()
    if last:
        dipoles, charges, far_table, wide = refs
    else:
        copies, rows, table, far_table, wide = refs
    fields, potential = far_terms(far, far_table, wide, first_cell + core, own)
    for b in range(AB):
        pol = own[POL + b : POL + b + 1, :]
        for a in range(3):
            r = a * AB + b
            value = pol * (own[FIXED + r : FIXED + r + 1, :] + (near[r : r + 1, :] + fields[b][a]))
            if last:
                dipoles[a : a + 1, b * LANES : (b + 1) * LANES] = value
            else:
                rows[r : r + 1, :] = value
    for b in range(GB):
        value = own[BASE + b : BASE + b + 1, :] - own[RESP + b : RESP + b + 1, :] * (
            near[12 + b : 13 + b, :] + potential[b]
        )
        if last:
            charges[b * LANES : (b + 1) * LANES] = value[0]
        else:
            rows[12 + b : 13 + b, :] = value
    if not last:
        share_sums(rows, own, table)
        everything = rows[...]
        for i in range(MEMBERS):
            copies[i] = everything


def columns():
    return [[chip * MEMBERS + m for m in reversed(range(MEMBERS))] for chip in range(CHIPS)]


def planes():
    return [[chip * MEMBERS + m for chip in reversed(range(CHIPS))] for m in range(MEMBERS)]


def swaps():
    pairs = []
    for c in range(1, CHIPS * CORES - 1, 2):
        for g in range(GROUPS):
            i, j = c * GROUPS + g, (c + 1) * GROUPS + g
            pairs += [(i, j), (j, i)]
    return pairs


def begin(sites, points, guess, fixed, pol, base, resp):
    return call(
        begin_kernel,
        (out(OWN, LANES), out(MEMBERS, FIRST, LANES)),
        (sites, points, guess, fixed, pol, base, resp),
        specs=[ANY] * 7,
        scratch=[
            pltpu.VMEM((FIRST, LANES), jnp.float32),
            pltpu.VMEM((8, LANES), jnp.float32),
            pltpu.VMEM((3, AB * LANES), jnp.float32),
            pltpu.VMEM((3, GB * LANES), jnp.float32),
            pltpu.VMEM((3, AB * LANES), jnp.float32),
            pltpu.VMEM((3, AB * LANES), jnp.float32),
            pltpu.SemaphoreType.DMA((4 + AB + 2 * GB,)),
        ],
        limit=60 << 20,
    )


def body(sites, points, guess, fixed, pol, base, resp, near, grids, sources):
    own, copies = begin(sites, points, guess, fixed, pol, base, resp)
    far_scratch = [
        pltpu.VMEM((CHIPS, LANES), jnp.float32),
        pltpu.VMEM((7 * VECTORS, 8, LANES), jnp.float32),
    ]
    static = static_halo = None
    every = ("x", "z", "core", "grp")
    for iteration in range(ITERS):
        last = iteration == ITERS - 1
        height = FIRST if iteration == 0 else DYN
        dyn = lax.all_to_all(copies, every, 0, 0, axis_index_groups=columns(), tiled=True)
        static = dyn if static is None else static
        far_out, halo_out = call(
            sums_kernel, (out(CHIPS, 1, LANES), out(GROUPS, height, LANES)), (dyn,)
        )
        halo = lax.ppermute(halo_out, every, swaps())
        far = lax.all_to_all(far_out, every, 0, 0, axis_index_groups=planes(), tiled=True)
        static_halo = halo if static_halo is None else static_halo
        near_field = call(
            near_kernel,
            out(16, LANES),
            (near, grids, sources, own, dyn, halo, static, static_halo),
            specs=[SM] * 3 + [VM] * 5,
            flops=40_000_000,
            scratch=[
                pltpu.VMEM((21, LANES, LANES), jnp.float32),
                pltpu.VMEM((15, LANES, LANES), jnp.float32),
                pltpu.VMEM((MEMBERS + GROUPS, DYN, LANES), jnp.float32),
                pltpu.VMEM((MEMBERS + GROUPS, FIRST - SITE, LANES), jnp.float32),
            ],
            limit=16 << 20,
        )
        if last:
            dipoles, charges = call(
                functools.partial(update_kernel, True),
                (out(3, AB * LANES), out(GB * LANES)),
                (own, near_field, far),
                scratch=far_scratch,
            )
        else:
            copies = call(
                functools.partial(update_kernel, False),
                out(MEMBERS, DYN, LANES),
                (own, near_field, far),
                scratch=[pltpu.VMEM((DYN, LANES), jnp.float32), pltpu.VMEM((8, LANES), jnp.float32)]
                + far_scratch,
            )
    return dipoles, charges


def solution(mesh):
    fine = Mesh(mesh.devices.reshape(X, Z, CORES, GROUPS), ("x", "z", "core", "grp"))
    every = ("x", "z", "core", "grp")
    return jax.shard_map(
        body,
        mesh=fine,
        in_specs=(P(None, every),) * 4 + (P(every),) * 3 + (P(every, None),) * 3,
        out_specs=(P(None, every), P(every)),
        check_vma=False,
    )
```

```python
import functools

import jax
import jax.numpy as jnp
from jax import lax
from jax.experimental import pallas as pl
from jax.experimental.pallas import tpu as pltpu
from jax.sharding import Mesh, PartitionSpec as P


LANES = 128
ITERS = 3
SOFT = 0.04
X, Z, CORES, GROUPS = 4, 8, 2, 8
CHIPS = X * Z
MEMBERS = CORES * GROUPS
AB, GB = 4, 3
DYN = 16
FIRST = 40
SITE, POINT = 16, 28
OWN = 48
FIXED, POL, BASE, RESP = 21, 33, 37, 40

VM = pl.BlockSpec(memory_space=pltpu.VMEM)
SM = pl.BlockSpec(memory_space=pltpu.SMEM)
ANY = pl.BlockSpec(memory_space=pl.ANY)


def out(*shape):
    return jax.ShapeDtypeStruct(shape, jnp.float32)


def call(kernel, outs, args, specs=None, flops=1_000_000, scratch=(), limit=8 << 20):
    return pl.pallas_call(
        kernel,
        out_shape=outs,
        in_specs=specs or [VM] * len(args),
        out_specs=jax.tree.map(lambda _: VM, outs),
        scratch_shapes=list(scratch),
        cost_estimate=pl.CostEstimate(flops=flops, bytes_accessed=1000, transcendentals=0),
        compiler_params=pltpu.CompilerParams(vmem_limit_bytes=limit),
    )(*args)


def share_sums(rows, own, table):
    core, first_cell = position()
    centre = [(first_cell + core).astype(jnp.float32) + 0.5, 0.5, 0.5]
    q = rows[12 : 12 + GB, :]
    table[7:8, :] = jnp.zeros((1, LANES), jnp.float32)
    table[3:4, :] = jnp.sum(q, axis=0, keepdims=True)
    for a in range(3):
        p = jnp.sum(rows[a * AB : (a + 1) * AB, :], axis=0, keepdims=True)
        d = q * (own[12 + a * GB : 12 + (a + 1) * GB, :] - centre[a])
        table[a : a + 1, :] = p
        table[4 + a : 5 + a, :] = p + jnp.sum(d, axis=0, keepdims=True)
    totals = jnp.broadcast_to(jnp.sum(table[...], axis=1, keepdims=True), (8, LANES))
    lane = lax.broadcasted_iota(jnp.int32, (8, LANES), 1)
    chosen = (lax.broadcasted_iota(jnp.int32, (8, LANES), 0) == (lane & 7)) & (lane < 16)
    rows[15:16, :] = jnp.sum(jnp.where(chosen, totals, 0.0), axis=0, keepdims=True)


def begin_kernel(
    sites, points, guess, fixed, pol, base, resp, own, copies, rows, table, in_sites, in_points, in_guess, in_fixed, sems
):
    pieces = [(sites, in_sites), (points, in_points), (guess, in_guess), (fixed, in_fixed)]
    for b in range(AB):
        pieces.append((pol.at[pl.ds(b * LANES, LANES)], own.at[POL + b]))
    for b in range(GB):
        pieces.append((base.at[pl.ds(b * LANES, LANES)], own.at[BASE + b]))
        pieces.append((resp.at[pl.ds(b * LANES, LANES)], own.at[RESP + b]))
    moves = [pltpu.make_async_copy(src, dst, sems.at[i]) for i, (src, dst) in enumerate(pieces)]
    for move in moves:
        move.start()
    rows[37:40, :] = jnp.zeros((3, LANES), jnp.float32)
    own[43:48, :] = jnp.zeros((5, LANES), jnp.float32)
    for move in moves:
        move.wait()
    for b in range(AB):
        lanes = slice(b * LANES, (b + 1) * LANES)
        for a in range(3):
            r = a * AB + b
            s = in_sites[a : a + 1, lanes]
            rows[r : r + 1, :] = in_guess[a : a + 1, lanes]
            rows[SITE + r : SITE + r + 1, :] = s
            own[r : r + 1, :] = s
            own[FIXED + r : FIXED + r + 1, :] = in_fixed[a : a + 1, lanes]
    for b in range(GB):
        lanes = slice(b * LANES, (b + 1) * LANES)
        for a in range(3):
            r = a * GB + b
            s = in_points[a : a + 1, lanes]
            rows[POINT + r : POINT + r + 1, :] = s
            own[12 + r : 13 + r, :] = s
        rows[12 + b : 13 + b, :] = own[BASE + b : BASE + b + 1, :]
    share_sums(rows, own, table)
    everything = rows[...]
    for i in range(MEMBERS):
        copies[i] = everything


def position():
    core = lax.axis_index("core")
    return core, (lax.axis_index("x") * Z + lax.axis_index("z")) * CORES


def sums_kernel(dyn, far, halo):
    core, _ = position()
    totals = []
    for k in range(CORES):
        total = None
        for g in range(GROUPS):
            part = dyn[place_of(k, g), 15:16, :]
            total = part if total is None else total + part
        totals.append(total)
    lane = lax.broadcasted_iota(jnp.int32, (1, LANES), 1)
    row = jnp.where(lane < 8, totals[0], totals[1])
    for i in range(CHIPS):
        far[i] = row
    for g in range(GROUPS):
        halo[g] = dyn[place_of(core, g)]


def geometry(t, s):
    dx, dy, dz = (t[a] - s[a] for a in range(3))
    inverse = lax.rsqrt(dx * dx + dy * dy + (dz * dz + SOFT))
    square = inverse * inverse
    return dx, dy, dz, inverse * square, square


CHUNK = 128


def near_kernel(
    lists, own, dyn, dyn_halo, static, static_halo, result, columns, sums, moving, fixed
):
    core, _ = position()
    for m in range(MEMBERS):
        at = place_of(m // GROUPS, m % GROUPS)
        moving[m] = dyn[at, 0:DYN, :]
        fixed[m] = static[at, SITE:FIRST, :]
    for g in range(GROUPS):
        moving[MEMBERS + g] = dyn_halo[g, 0:DYN, :]
        fixed[MEMBERS + g] = static_halo[g, SITE:FIRST, :]
    for r in range(3 * AB + 3 * GB):
        columns[r] = jnp.transpose(jnp.broadcast_to(own[r : r + 1, :], (LANES, LANES)))

    first, second, third = (
        jnp.where(core == 0, MEMBERS, 0),
        jnp.where(core == 0, 0, GROUPS),
        jnp.where(core == 0, GROUPS, MEMBERS),
    )

    def place(slot, blocks):
        per_cell = blocks * GROUPS
        cell = slot // per_cell
        inside = slot - cell * per_cell
        share = jnp.where(cell == 0, first, jnp.where(cell == 1, second, third))
        group = inside // blocks
        return share + group, inside - group * blocks

    def rows(ref, share, start, step):
        return [ref[share, pl.ds(start + a * step, 1), :] for a in range(3)]

    def dipole_terms(share, b):
        s = rows(fixed, share, b, AB)
        m = rows(moving, share, b, AB)
        return s, m, [3.0 * v for v in m]

    me = second + lax.axis_index("grp")

    def finished(r):
        result[r : r + 1, :] = jnp.sum(jnp.transpose(sums[r]), axis=0, keepdims=True)

    def atom_chunk(step, carry):
        tb = step // (LANES // CHUNK)
        start = 0
        t = [columns[a * AB + tb, pl.ds(start, CHUNK), :] for a in range(3)]
        acc = [jnp.zeros((CHUNK, LANES), jnp.float32) for _ in range(3)]
        for n in range(9):
            if n == 0:
                share, b = me, tb
            else:
                share, b = place(lists[tb, n - 1], AB)
            s, m, m3 = dipole_terms(share, b)
            dx, dy, dz, cube, square = geometry(t, s)
            weight = (m3[0] * dx + m3[1] * dy + m3[2] * dz) * (cube * square)
            if n == 0:
                other = (
                    lax.broadcasted_iota(jnp.int32, (CHUNK, LANES), 0) + start
                ) != lax.broadcasted_iota(jnp.int32, (CHUNK, LANES), 1)
                cube = jnp.where(other, cube, 0.0)
                weight = jnp.where(other, weight, 0.0)
            acc = [acc[a] + (weight * d - m[a] * cube) for a, d in enumerate((dx, dy, dz))]
        for n in range(4):
            share, b = place(lists[AB + tb, n], GB)
            s = rows(fixed, share, 12 + b, GB)
            q = moving[share, pl.ds(12 + b, 1), :]
            dx, dy, dz, cube, _ = geometry(t, s)
            weight = q * cube
            acc = [acc[a] + weight * d for a, d in enumerate((dx, dy, dz))]
        for a in range(3):
            sums[a * AB + tb, pl.ds(start, CHUNK), :] = acc[a]
        return carry

    def grid_chunk(step, carry):
        tb = step // (LANES // CHUNK)
        start = 0
        t = [columns[12 + a * GB + tb, pl.ds(start, CHUNK), :] for a in range(3)]
        acc = jnp.zeros((CHUNK, LANES), jnp.float32)
        for n in range(8):
            share, b = place(lists[2 * AB + tb, n], AB)
            s = rows(fixed, share, b, AB)
            m = rows(moving, share, b, AB)
            dx, dy, dz, cube, _ = geometry(t, s)
            acc = acc + (m[0] * dx + m[1] * dy + m[2] * dz) * cube
        sums[12 + tb, pl.ds(start, CHUNK), :] = acc
        return carry

    for step in range(AB):
        atom_chunk(step, 0)
        for a in range(3):
            finished(a * AB + step)
    for step in range(GB):
        grid_chunk(step, 0)
        finished(12 + step)
    result[15:16, :] = jnp.zeros((1, LANES), jnp.float32)


VECTORS = CORES * CHIPS // 8


def far_terms(far, table, wide, here, own):
    for i in range(CHIPS):
        table[i : i + 1, :] = far[CHIPS - 1 - i]
    centres, masks = [], []
    for n in range(VECTORS):
        k, v = n // (CHIPS // 8), n % (CHIPS // 8)
        cell = (lax.broadcasted_iota(jnp.int32, (8, LANES), 0) + v * 8) * CORES + k
        centres.append(cell.astype(jnp.float32) + 0.5)
        masks.append(jnp.where(jnp.abs(cell - here) >= 2, 1.0, 0.0))
        part = table[v * 8 : (v + 1) * 8, :]
        for j in range(7):
            wide[n * 7 + j] = jnp.broadcast_to(part[:, k * 8 + j : k * 8 + j + 1], (8, LANES))

    def wide_row(r):
        return jnp.broadcast_to(own[r : r + 1, :], (8, LANES))

    fields, potential = [], []
    for b in range(AB + GB):
        atom = b < AB
        r, stride = (b, AB) if atom else (12 + b - AB, GB)
        x, dy, dz = wide_row(r), wide_row(r + stride) - 0.5, wide_row(r + 2 * stride) - 0.5
        across = dy * dy + (dz * dz + SOFT)
        sums = None
        for n in range(VECTORS):
            dx = x - centres[n]
            inverse = lax.rsqrt(dx * dx + across)
            square = inverse * inverse
            cube = inverse * square * masks[n]
            if atom:
                q, m0, m1, m2 = (wide[n * 7 + j] for j in (3, 4, 5, 6))
                weight = 3.0 * (m0 * dx + m1 * dy + m2 * dz) * (cube * square) + q * cube
                terms = [weight * dx - m0 * cube, m1 * cube, m2 * cube, weight]
            else:
                p0, p1, p2 = (wide[n * 7 + j] for j in (0, 1, 2))
                terms = [(p0 * dx + p1 * dy + p2 * dz) * cube]
            sums = terms if sums is None else [s + t for s, t in zip(sums, terms)]
        if atom:
            sx, sy, sz, sw = sums
            parts = [sx, dy * sw - sy, dz * sw - sz]
            fields.append([jnp.sum(t, axis=0, keepdims=True) for t in parts])
        else:
            potential.append(jnp.sum(sums[0], axis=0, keepdims=True))
    return fields, potential


def update_kernel(last, own, near, far, *refs):
    core, first_cell = position()
    if last:
        dipoles, charges, far_table, wide = refs
    else:
        copies, rows, table, far_table, wide = refs
    fields, potential = far_terms(far, far_table, wide, first_cell + core, own)
    for b in range(AB):
        pol = own[POL + b : POL + b + 1, :]
        for a in range(3):
            r = a * AB + b
            value = pol * (own[FIXED + r : FIXED + r + 1, :] + (near[r : r + 1, :] + fields[b][a]))
            if last:
                dipoles[a : a + 1, b * LANES : (b + 1) * LANES] = value
            else:
                rows[r : r + 1, :] = value
    for b in range(GB):
        value = own[BASE + b : BASE + b + 1, :] - own[RESP + b : RESP + b + 1, :] * (
            near[12 + b : 13 + b, :] + potential[b]
        )
        if last:
            charges[b * LANES : (b + 1) * LANES] = value[0]
        else:
            rows[12 + b : 13 + b, :] = value
    if not last:
        share_sums(rows, own, table)
        everything = rows[...]
        for i in range(MEMBERS):
            copies[i] = everything


def columns():
    order = [k * GROUPS + g for g in reversed(range(GROUPS)) for k in reversed(range(CORES))]
    return [[chip * MEMBERS + m for m in order] for chip in range(CHIPS)]


def place_of(core, group):
    return (GROUPS - 1 - group) * CORES + (CORES - 1 - core)


def planes():
    return [[chip * MEMBERS + m for chip in reversed(range(CHIPS))] for m in range(MEMBERS)]


def swaps():
    pairs = []
    for c in range(1, CHIPS * CORES - 1, 2):
        for g in range(GROUPS):
            i, j = c * GROUPS + g, (c + 1) * GROUPS + g
            pairs += [(i, j), (j, i)]
    return pairs


def begin(sites, points, guess, fixed, pol, base, resp):
    return call(
        begin_kernel,
        (out(OWN, LANES), out(MEMBERS, FIRST, LANES)),
        (sites, points, guess, fixed, pol, base, resp),
        specs=[ANY] * 7,
        scratch=[
            pltpu.VMEM((FIRST, LANES), jnp.float32),
            pltpu.VMEM((8, LANES), jnp.float32),
            pltpu.VMEM((3, AB * LANES), jnp.float32),
            pltpu.VMEM((3, GB * LANES), jnp.float32),
            pltpu.VMEM((3, AB * LANES), jnp.float32),
            pltpu.VMEM((3, AB * LANES), jnp.float32),
            pltpu.SemaphoreType.DMA((4 + AB + 2 * GB,)),
        ],
        limit=60 << 20,
    )


def body(sites, points, guess, fixed, pol, base, resp, near, grids, sources):
    own, copies = begin(sites, points, guess, fixed, pol, base, resp)
    far_scratch = [
        pltpu.VMEM((CHIPS, LANES), jnp.float32),
        pltpu.VMEM((7 * VECTORS, 8, LANES), jnp.float32),
    ]
    static = static_halo = None
    lists = jnp.concatenate([near, jnp.pad(grids, ((0, 0), (0, 4))), sources])
    every = ("x", "z", "core", "grp")
    for iteration in range(ITERS):
        last = iteration == ITERS - 1
        height = FIRST if iteration == 0 else DYN
        dyn = lax.all_to_all(copies, every, 0, 0, axis_index_groups=columns(), tiled=True)
        static = dyn if static is None else static
        far_out, halo_out = call(
            sums_kernel, (out(CHIPS, 1, LANES), out(GROUPS, height, LANES)), (dyn,)
        )
        halo = lax.ppermute(halo_out, every, swaps())
        far = lax.all_to_all(far_out, every, 0, 0, axis_index_groups=planes(), tiled=True)
        static_halo = halo if static_halo is None else static_halo
        near_field = call(
            near_kernel,
            out(16, LANES),
            (lists, own, dyn, halo, static, static_halo),
            specs=[SM] + [VM] * 5,
            flops=40_000_000,
            scratch=[
                pltpu.VMEM((21, LANES, LANES), jnp.float32),
                pltpu.VMEM((15, LANES, LANES), jnp.float32),
                pltpu.VMEM((MEMBERS + GROUPS, DYN, LANES), jnp.float32),
                pltpu.VMEM((MEMBERS + GROUPS, FIRST - SITE, LANES), jnp.float32),
            ],
            limit=16 << 20,
        )
        if last:
            dipoles, charges = call(
                functools.partial(update_kernel, True),
                (out(3, AB * LANES), out(GB * LANES)),
                (own, near_field, far),
                scratch=far_scratch,
            )
        else:
            copies = call(
                functools.partial(update_kernel, False),
                out(MEMBERS, DYN, LANES),
                (own, near_field, far),
                scratch=[pltpu.VMEM((DYN, LANES), jnp.float32), pltpu.VMEM((8, LANES), jnp.float32)]
                + far_scratch,
            )
    return dipoles, charges


def solution(mesh):
    fine = Mesh(mesh.devices.reshape(X, Z, CORES, GROUPS), ("x", "z", "core", "grp"))
    every = ("x", "z", "core", "grp")
    return jax.shard_map(
        body,
        mesh=fine,
        in_specs=(P(None, every),) * 4 + (P(every),) * 3 + (P(every, None),) * 3,
        out_specs=(P(None, every), P(every)),
        check_vma=False,
    )
```

```python
import functools

import jax
import jax.numpy as jnp
from jax import lax
from jax.experimental import pallas as pl
from jax.experimental.pallas import tpu as pltpu
from jax.sharding import Mesh, PartitionSpec as P


LANES = 128
ITERS = 3
SOFT = 0.04
X, Z, CORES, GROUPS = 4, 8, 2, 8
CHIPS = X * Z
MEMBERS = CORES * GROUPS
AB, GB = 4, 3
DYN = 16
FIRST = 40
SITE, POINT = 16, 28
OWN = 48
FIXED, POL, BASE, RESP = 21, 33, 37, 40

VM = pl.BlockSpec(memory_space=pltpu.VMEM)
SM = pl.BlockSpec(memory_space=pltpu.SMEM)
ANY = pl.BlockSpec(memory_space=pl.ANY)


def out(*shape):
    return jax.ShapeDtypeStruct(shape, jnp.float32)


def call(kernel, outs, args, specs=None, flops=1_000_000, scratch=(), limit=8 << 20):
    return pl.pallas_call(
        kernel,
        out_shape=outs,
        in_specs=specs or [VM] * len(args),
        out_specs=jax.tree.map(lambda _: VM, outs),
        scratch_shapes=list(scratch),
        cost_estimate=pl.CostEstimate(flops=flops, bytes_accessed=1000, transcendentals=0),
        compiler_params=pltpu.CompilerParams(vmem_limit_bytes=limit),
    )(*args)


def share_sums(rows, own, table):
    core, first_cell = position()
    centre = [(first_cell + core).astype(jnp.float32) + 0.5, 0.5, 0.5]
    q = rows[12 : 12 + GB, :]
    table[7:8, :] = jnp.zeros((1, LANES), jnp.float32)
    table[3:4, :] = jnp.sum(q, axis=0, keepdims=True)
    for a in range(3):
        p = jnp.sum(rows[a * AB : (a + 1) * AB, :], axis=0, keepdims=True)
        d = q * (own[12 + a * GB : 12 + (a + 1) * GB, :] - centre[a])
        table[a : a + 1, :] = p
        table[4 + a : 5 + a, :] = p + jnp.sum(d, axis=0, keepdims=True)
    totals = jnp.broadcast_to(jnp.sum(table[...], axis=1, keepdims=True), (8, LANES))
    lane = lax.broadcasted_iota(jnp.int32, (8, LANES), 1)
    chosen = (lax.broadcasted_iota(jnp.int32, (8, LANES), 0) == (lane & 7)) & (lane < 16)
    rows[15:16, :] = jnp.sum(jnp.where(chosen, totals, 0.0), axis=0, keepdims=True)


def begin_kernel(
    sites, points, guess, fixed, pol, base, resp, own, copies, rows, table, in_sites, in_points, in_guess, in_fixed, sems
):
    pieces = [(sites, in_sites), (points, in_points), (guess, in_guess), (fixed, in_fixed)]
    for b in range(AB):
        pieces.append((pol.at[pl.ds(b * LANES, LANES)], own.at[POL + b]))
    for b in range(GB):
        pieces.append((base.at[pl.ds(b * LANES, LANES)], own.at[BASE + b]))
        pieces.append((resp.at[pl.ds(b * LANES, LANES)], own.at[RESP + b]))
    moves = [pltpu.make_async_copy(src, dst, sems.at[i]) for i, (src, dst) in enumerate(pieces)]
    for move in moves:
        move.start()
    rows[37:40, :] = jnp.zeros((3, LANES), jnp.float32)
    own[43:48, :] = jnp.zeros((5, LANES), jnp.float32)
    for move in moves:
        move.wait()
    for b in range(AB):
        lanes = slice(b * LANES, (b + 1) * LANES)
        for a in range(3):
            r = a * AB + b
            s = in_sites[a : a + 1, lanes]
            rows[r : r + 1, :] = in_guess[a : a + 1, lanes]
            rows[SITE + r : SITE + r + 1, :] = s
            own[r : r + 1, :] = s
            own[FIXED + r : FIXED + r + 1, :] = in_fixed[a : a + 1, lanes]
    for b in range(GB):
        lanes = slice(b * LANES, (b + 1) * LANES)
        for a in range(3):
            r = a * GB + b
            s = in_points[a : a + 1, lanes]
            rows[POINT + r : POINT + r + 1, :] = s
            own[12 + r : 13 + r, :] = s
        rows[12 + b : 13 + b, :] = own[BASE + b : BASE + b + 1, :]
    share_sums(rows, own, table)
    everything = rows[...]
    for i in range(MEMBERS):
        copies[i] = everything


def position():
    core = lax.axis_index("core")
    return core, (lax.axis_index("x") * Z + lax.axis_index("z")) * CORES


def sums_kernel(dyn, far, halo):
    core, _ = position()
    totals = []
    for k in range(CORES):
        total = None
        for g in range(GROUPS):
            part = dyn[place_of(k, g), 15:16, :]
            total = part if total is None else total + part
        totals.append(total)
    lane = lax.broadcasted_iota(jnp.int32, (1, LANES), 1)
    row = jnp.where(lane < 8, totals[0], totals[1])
    for i in range(CHIPS):
        far[i] = row
    for g in range(GROUPS):
        halo[g] = dyn[place_of(core, g)]


def geometry(t, s):
    dx, dy, dz = (t[a] - s[a] for a in range(3))
    inverse = lax.rsqrt(dx * dx + dy * dy + (dz * dz + SOFT))
    square = inverse * inverse
    return dx, dy, dz, inverse * square, square


CHUNK = 128


def near_kernel(
    given, own, dyn, dyn_halo, static, static_halo, result, columns, sums, moving, fixed, lists, sem
):
    move = pltpu.make_async_copy(given, lists, sem)
    move.start()
    core, _ = position()
    for m in range(MEMBERS):
        at = place_of(m // GROUPS, m % GROUPS)
        moving[m] = dyn[at, 0:DYN, :]
        fixed[m] = static[at, SITE:FIRST, :]
    for g in range(GROUPS):
        moving[MEMBERS + g] = dyn_halo[g, 0:DYN, :]
        fixed[MEMBERS + g] = static_halo[g, SITE:FIRST, :]
    for r in range(3 * AB + 3 * GB):
        columns[r] = jnp.transpose(jnp.broadcast_to(own[r : r + 1, :], (LANES, LANES)))

    first, second, third = (
        jnp.where(core == 0, MEMBERS, 0),
        jnp.where(core == 0, 0, GROUPS),
        jnp.where(core == 0, GROUPS, MEMBERS),
    )

    def place(slot, blocks):
        per_cell = blocks * GROUPS
        cell = slot // per_cell
        inside = slot - cell * per_cell
        share = jnp.where(cell == 0, first, jnp.where(cell == 1, second, third))
        group = inside // blocks
        return share + group, inside - group * blocks

    def rows(ref, share, start, step):
        return [ref[share, pl.ds(start + a * step, 1), :] for a in range(3)]

    def dipole_terms(share, b):
        s = rows(fixed, share, b, AB)
        m = rows(moving, share, b, AB)
        return s, m, [3.0 * v for v in m]

    me = second + lax.axis_index("grp")
    move.wait()

    def finished(r):
        result[r : r + 1, :] = jnp.sum(jnp.transpose(sums[r]), axis=0, keepdims=True)

    def atom_chunk(step, carry):
        tb = step // (LANES // CHUNK)
        start = 0
        t = [columns[a * AB + tb, pl.ds(start, CHUNK), :] for a in range(3)]
        acc = [jnp.zeros((CHUNK, LANES), jnp.float32) for _ in range(3)]
        for n in range(9):
            if n == 0:
                share, b = me, tb
            else:
                share, b = place(lists[tb, n - 1], AB)
            s, m, m3 = dipole_terms(share, b)
            dx, dy, dz, cube, square = geometry(t, s)
            weight = (m3[0] * dx + m3[1] * dy + m3[2] * dz) * (cube * square)
            if n == 0:
                other = (
                    lax.broadcasted_iota(jnp.int32, (CHUNK, LANES), 0) + start
                ) != lax.broadcasted_iota(jnp.int32, (CHUNK, LANES), 1)
                cube = jnp.where(other, cube, 0.0)
                weight = jnp.where(other, weight, 0.0)
            acc = [acc[a] + (weight * d - m[a] * cube) for a, d in enumerate((dx, dy, dz))]
        for n in range(4):
            share, b = place(lists[AB + tb, n], GB)
            s = rows(fixed, share, 12 + b, GB)
            q = moving[share, pl.ds(12 + b, 1), :]
            dx, dy, dz, cube, _ = geometry(t, s)
            weight = q * cube
            acc = [acc[a] + weight * d for a, d in enumerate((dx, dy, dz))]
        for a in range(3):
            sums[a * AB + tb, pl.ds(start, CHUNK), :] = acc[a]
        return carry

    def grid_chunk(step, carry):
        tb = step // (LANES // CHUNK)
        start = 0
        t = [columns[12 + a * GB + tb, pl.ds(start, CHUNK), :] for a in range(3)]
        acc = jnp.zeros((CHUNK, LANES), jnp.float32)
        for n in range(8):
            share, b = place(lists[2 * AB + tb, n], AB)
            s = rows(fixed, share, b, AB)
            m = rows(moving, share, b, AB)
            dx, dy, dz, cube, _ = geometry(t, s)
            acc = acc + (m[0] * dx + m[1] * dy + m[2] * dz) * cube
        sums[12 + tb, pl.ds(start, CHUNK), :] = acc
        return carry

    for step in range(AB):
        atom_chunk(step, 0)
        for a in range(3):
            finished(a * AB + step)
    for step in range(GB):
        grid_chunk(step, 0)
        finished(12 + step)
    result[15:16, :] = jnp.zeros((1, LANES), jnp.float32)


VECTORS = CORES * CHIPS // 8


def far_terms(far, table, wide, here, own):
    for i in range(CHIPS):
        table[i : i + 1, :] = far[CHIPS - 1 - i]
    centres, masks = [], []
    for n in range(VECTORS):
        k, v = n // (CHIPS // 8), n % (CHIPS // 8)
        cell = (lax.broadcasted_iota(jnp.int32, (8, LANES), 0) + v * 8) * CORES + k
        centres.append(cell.astype(jnp.float32) + 0.5)
        masks.append(jnp.where(jnp.abs(cell - here) >= 2, 1.0, 0.0))
        part = table[v * 8 : (v + 1) * 8, :]
        for j in range(7):
            wide[n * 7 + j] = jnp.broadcast_to(part[:, k * 8 + j : k * 8 + j + 1], (8, LANES))

    def wide_row(r):
        return jnp.broadcast_to(own[r : r + 1, :], (8, LANES))

    fields, potential = [], []
    for b in range(AB + GB):
        atom = b < AB
        r, stride = (b, AB) if atom else (12 + b - AB, GB)
        x, dy, dz = wide_row(r), wide_row(r + stride) - 0.5, wide_row(r + 2 * stride) - 0.5
        across = dy * dy + (dz * dz + SOFT)
        sums = None
        for n in range(VECTORS):
            dx = x - centres[n]
            inverse = lax.rsqrt(dx * dx + across)
            square = inverse * inverse
            cube = inverse * square * masks[n]
            if atom:
                q, m0, m1, m2 = (wide[n * 7 + j] for j in (3, 4, 5, 6))
                weight = 3.0 * (m0 * dx + m1 * dy + m2 * dz) * (cube * square) + q * cube
                terms = [weight * dx - m0 * cube, m1 * cube, m2 * cube, weight]
            else:
                p0, p1, p2 = (wide[n * 7 + j] for j in (0, 1, 2))
                terms = [(p0 * dx + p1 * dy + p2 * dz) * cube]
            sums = terms if sums is None else [s + t for s, t in zip(sums, terms)]
        if atom:
            sx, sy, sz, sw = sums
            parts = [sx, dy * sw - sy, dz * sw - sz]
            fields.append([jnp.sum(t, axis=0, keepdims=True) for t in parts])
        else:
            potential.append(jnp.sum(sums[0], axis=0, keepdims=True))
    return fields, potential


def update_kernel(last, own, near, far, *refs):
    core, first_cell = position()
    if last:
        dipoles, charges, far_table, wide = refs
    else:
        copies, rows, table, far_table, wide = refs
    fields, potential = far_terms(far, far_table, wide, first_cell + core, own)
    for b in range(AB):
        pol = own[POL + b : POL + b + 1, :]
        for a in range(3):
            r = a * AB + b
            value = pol * (own[FIXED + r : FIXED + r + 1, :] + (near[r : r + 1, :] + fields[b][a]))
            if last:
                dipoles[a : a + 1, b * LANES : (b + 1) * LANES] = value
            else:
                rows[r : r + 1, :] = value
    for b in range(GB):
        value = own[BASE + b : BASE + b + 1, :] - own[RESP + b : RESP + b + 1, :] * (
            near[12 + b : 13 + b, :] + potential[b]
        )
        if last:
            charges[b * LANES : (b + 1) * LANES] = value[0]
        else:
            rows[12 + b : 13 + b, :] = value
    if not last:
        share_sums(rows, own, table)
        everything = rows[...]
        for i in range(MEMBERS):
            copies[i] = everything


def columns():
    order = [k * GROUPS + g for g in reversed(range(GROUPS)) for k in reversed(range(CORES))]
    return [[chip * MEMBERS + m for m in order] for chip in range(CHIPS)]


def place_of(core, group):
    return (GROUPS - 1 - group) * CORES + (CORES - 1 - core)


def planes():
    return [[chip * MEMBERS + m for chip in reversed(range(CHIPS))] for m in range(MEMBERS)]


def swaps():
    pairs = []
    for c in range(1, CHIPS * CORES - 1, 2):
        for g in range(GROUPS):
            i, j = c * GROUPS + g, (c + 1) * GROUPS + g
            pairs += [(i, j), (j, i)]
    return pairs


def begin(sites, points, guess, fixed, pol, base, resp):
    return call(
        begin_kernel,
        (out(OWN, LANES), out(MEMBERS, FIRST, LANES)),
        (sites, points, guess, fixed, pol, base, resp),
        specs=[ANY] * 7,
        scratch=[
            pltpu.VMEM((FIRST, LANES), jnp.float32),
            pltpu.VMEM((8, LANES), jnp.float32),
            pltpu.VMEM((3, AB * LANES), jnp.float32),
            pltpu.VMEM((3, GB * LANES), jnp.float32),
            pltpu.VMEM((3, AB * LANES), jnp.float32),
            pltpu.VMEM((3, AB * LANES), jnp.float32),
            pltpu.SemaphoreType.DMA((4 + AB + 2 * GB,)),
        ],
        limit=60 << 20,
    )


def body(sites, points, guess, fixed, pol, base, resp, near, grids, sources):
    own, copies = begin(sites, points, guess, fixed, pol, base, resp)
    far_scratch = [
        pltpu.VMEM((CHIPS, LANES), jnp.float32),
        pltpu.VMEM((7 * VECTORS, 8, LANES), jnp.float32),
    ]
    static = static_halo = None
    lists = jnp.concatenate([near, jnp.pad(grids, ((0, 0), (0, 4))), sources])
    every = ("x", "z", "core", "grp")
    for iteration in range(ITERS):
        last = iteration == ITERS - 1
        height = FIRST if iteration == 0 else DYN
        dyn = lax.all_to_all(copies, every, 0, 0, axis_index_groups=columns(), tiled=True)
        static = dyn if static is None else static
        far_out, halo_out = call(
            sums_kernel, (out(CHIPS, 1, LANES), out(GROUPS, height, LANES)), (dyn,)
        )
        halo = lax.ppermute(halo_out, every, swaps())
        far = lax.all_to_all(far_out, every, 0, 0, axis_index_groups=planes(), tiled=True)
        static_halo = halo if static_halo is None else static_halo
        near_field = call(
            near_kernel,
            out(16, LANES),
            (lists, own, dyn, halo, static, static_halo),
            specs=[ANY] + [VM] * 5,
            flops=40_000_000,
            scratch=[
                pltpu.VMEM((21, LANES, LANES), jnp.float32),
                pltpu.VMEM((15, LANES, LANES), jnp.float32),
                pltpu.VMEM((MEMBERS + GROUPS, DYN, LANES), jnp.float32),
                pltpu.VMEM((MEMBERS + GROUPS, FIRST - SITE, LANES), jnp.float32),
                pltpu.SMEM(lists.shape, jnp.int32),
                pltpu.SemaphoreType.DMA(()),
            ],
            limit=16 << 20,
        )
        if last:
            dipoles, charges = call(
                functools.partial(update_kernel, True),
                (out(3, AB * LANES), out(GB * LANES)),
                (own, near_field, far),
                scratch=far_scratch,
            )
        else:
            copies = call(
                functools.partial(update_kernel, False),
                out(MEMBERS, DYN, LANES),
                (own, near_field, far),
                scratch=[pltpu.VMEM((DYN, LANES), jnp.float32), pltpu.VMEM((8, LANES), jnp.float32)]
                + far_scratch,
            )
    return dipoles, charges


def solution(mesh):
    fine = Mesh(mesh.devices.reshape(X, Z, CORES, GROUPS), ("x", "z", "core", "grp"))
    every = ("x", "z", "core", "grp")
    return jax.shard_map(
        body,
        mesh=fine,
        in_specs=(P(None, every),) * 4 + (P(every),) * 3 + (P(every, None),) * 3,
        out_specs=(P(None, every), P(every)),
        check_vma=False,
    )
```
